32 devices in a mesh: rep: 2 (over x), dp: 16 (over y, z, core).
Axes of the slice: x: 2, y: 2, z: 4, core: 2. Of those that a mesh axis runs over, the one named last changes fastest.
Arguments:
- x: bfloat16 [32, 2048, 512], P(('rep', 'dp')), parts along dimension 0
- dy: bfloat16 [32, 2048, 512], P(('rep', 'dp')), parts along dimension 0
- wq: bfloat16 [2, 512, 512], P(None, 'dp')
- wk: bfloat16 [2, 512, 512], P(None, 'dp')
- wv: bfloat16 [2, 512, 512], P(None, 'dp')
- wo: bfloat16 [2, 512, 512], P(None, 'dp')
- w_gate: bfloat16 [2, 512, 2048], P(None, 'dp')
- w_up: bfloat16 [2, 512, 2048], P(None, 'dp')
- w_down: bfloat16 [2, 2048, 512], P(None, 'dp')
- m_wq: float32 [2, 512, 512], P(None, 'dp')
- m_wk: float32 [2, 512, 512], P(None, 'dp')
- m_wv: float32 [2, 512, 512], P(None, 'dp')
- m_wo: float32 [2, 512, 512], P(None, 'dp')
- m_w_gate: float32 [2, 512, 2048], P(None, 'dp')
- m_w_up: float32 [2, 512, 2048], P(None, 'dp')
- m_w_down: float32 [2, 2048, 512], P(None, 'dp')
- v_wq: float32 [2, 512, 512], P(None, 'dp')
- v_wk: float32 [2, 512, 512], P(None, 'dp')
- v_wv: float32 [2, 512, 512], P(None, 'dp')
- v_wo: float32 [2, 512, 512], P(None, 'dp')
- v_w_gate: float32 [2, 512, 2048], P(None, 'dp')
- v_w_up: float32 [2, 512, 2048], P(None, 'dp')
- v_w_down: float32 [2, 2048, 512], P(None, 'dp')
Outputs:
- output 1: bfloat16 [4, 512, 512], P('rep', 'dp'), parts along dimension 0
- output 2: bfloat16 [4, 512, 512], P('rep', 'dp'), parts along dimension 0
- output 3: bfloat16 [4, 512, 512], P('rep', 'dp'), parts along dimension 0
- output 4: bfloat16 [4, 512, 512], P('rep', 'dp'), parts along dimension 0
- output 5: bfloat16 [4, 512, 2048], P('rep', 'dp'), parts along dimension 0
- output 6: bfloat16 [4, 512, 2048], P('rep', 'dp'), parts along dimension 0
- output 7: bfloat16 [4, 2048, 512], P('rep', 'dp'), parts along dimension 0
- output 8: float32 [4, 512, 512], P('rep', 'dp'), parts along dimension 0
- output 9: float32 [4, 512, 512], P('rep', 'dp'), parts along dimension 0
- output 10: float32 [4, 512, 512], P('rep', 'dp'), parts along dimension 0
- output 11: float32 [4, 512, 512], P('rep', 'dp'), parts along dimension 0
- output 12: float32 [4, 512, 2048], P('rep', 'dp'), parts along dimension 0
- output 13: float32 [4, 512, 2048], P('rep', 'dp'), parts along dimension 0
- output 14: float32 [4, 2048, 512], P('rep', 'dp'), parts along dimension 0
- output 15: float32 [4, 512, 512], P('rep', 'dp'), parts along dimension 0
- output 16: float32 [4, 512, 512], P('rep', 'dp'), parts along dimension 0
- output 17: float32 [4, 512, 512], P('rep', 'dp'), parts along dimension 0
- output 18: float32 [4, 512, 512], P('rep', 'dp'), parts along dimension 0
- output 19: float32 [4, 512, 2048], P('rep', 'dp'), parts along dimension 0
- output 20: float32 [4, 512, 2048], P('rep', 'dp'), parts along dimension 0
- output 21: float32 [4, 2048, 512], P('rep', 'dp'), parts along dimension 0
There are 2 independent parts. The reference program is written for one: setup_inputs(seed, part) draws one part's arguments, and reference() takes and returns one part's arrays. A program takes and returns all parts, laid end to end along the dimension named above; an argument that names none is the same for every part.
All inputs are finite; a program needn't handle non-finite values.
Results may differ from the reference program's by a relative error of at most 0.0246.
Values are sent between devices in bfloat16 or wider.
A program may use at most 2 GiB of HBM per device.

```python
import jax
import jax.numpy as jnp
from jax import lax

SEQUENCES = 16
TOKENS = 2048
D = 512
HEADS = 2
KV_HEADS = 2
HEAD = 256
FF = 2048
LAYERS = 2
THETA = 10000
NAMES = ("wq", "wk", "wv", "wo", "w_gate", "w_up", "w_down")
SHAPES = {
    "wq": (LAYERS, D, HEADS * HEAD),
    "wk": (LAYERS, D, KV_HEADS * HEAD),
    "wv": (LAYERS, D, KV_HEADS * HEAD),
    "wo": (LAYERS, HEADS * HEAD, D),
    "w_gate": (LAYERS, D, FF),
    "w_up": (LAYERS, D, FF),
    "w_down": (LAYERS, FF, D),
}


def bump(key, n, height):
    away = (jnp.arange(n, dtype=jnp.int32) - jax.random.randint(key, (), 0, n, jnp.int32)) % n
    return jnp.where(away < n // 8, height, 1.0)


def together(key, own, strength):
    shared = jax.random.normal(key, own.shape[1:], jnp.float32)
    return (own + strength * shared) * lax.rsqrt(1 + strength * strength)


def setup_inputs(seed: int = 0, part: int = 0) -> dict:
    kx, kdy, ka, kb, kz, kf, kh, kl, *keys = jax.random.split(jax.random.key(seed), 8 + 3 * len(NAMES))
    kx, kdy, ka, kb = (jax.random.fold_in(k, part) for k in (kx, kdy, ka, kb))
    kw, km, kv = (keys[i::3] for i in range(3))
    shape = (SEQUENCES, TOKENS, D)
    much_x, much_dy = jax.random.uniform(kz, (2,), jnp.float32, 0.0, 1.0)
    loud = 2.0 ** jax.random.uniform(jax.random.fold_in(kz, 1), (), jnp.float32, -1.0, 2.0)
    layers = 2.0 ** jax.random.uniform(kl, (LAYERS, 1, 1), jnp.float32, -1.0, 1.0)
    times = {"wq": 1.0, "wk": 1.0, "wv": 2.0, "wo": layers, "w_gate": 1.0, "w_up": bump(kh, FF, 4.0), "w_down": layers}
    x = together(ka, jax.random.normal(kx, shape, jnp.float32), much_x) * bump(kf, D, 4.0)
    dy = together(kb, jax.random.normal(kdy, shape, jnp.float32), much_dy)
    drawn = {"x": x.astype(jnp.bfloat16), "dy": (loud * dy * (SEQUENCES * TOKENS) ** -0.5).astype(jnp.bfloat16)}
    for key, name in zip(kw, NAMES, strict=True):
        drawn[name] = (jax.random.normal(key, SHAPES[name], jnp.float32) * SHAPES[name][1] ** -0.5 * times[name]).astype(jnp.bfloat16)
    for key, name in zip(km, NAMES, strict=True):
        drawn[f"m_{name}"] = 0.1 * jax.random.normal(key, SHAPES[name], jnp.float32)
    for key, name in zip(kv, NAMES, strict=True):
        drawn[f"v_{name}"] = loud * loud * jax.random.uniform(key, SHAPES[name], jnp.float32, 0.2, 0.6)
    return drawn


def matmul(a, w):
    return jnp.dot(a, w, preferred_element_type=jnp.float32).astype(jnp.bfloat16)


def normed(h):
    wide = h.astype(jnp.float32)
    scale = lax.rsqrt(jnp.mean(wide**2, -1, keepdims=True) + 1e-6)
    return (wide * scale).astype(jnp.bfloat16)


def turned(t, theta):
    half = t.shape[-1] // 2
    angle = jnp.arange(t.shape[0], dtype=jnp.float32)[:, None] * theta ** (-jnp.arange(half, dtype=jnp.float32) / half)
    cos, sin = jnp.cos(angle)[:, None], jnp.sin(angle)[:, None]
    a, b = t[..., :half].astype(jnp.float32), t[..., half:].astype(jnp.float32)
    return jnp.concatenate([a * cos - b * sin, b * cos + a * sin], -1).astype(jnp.bfloat16)


def seen_by(q, k, v):
    tokens, kv = q.shape[0], k.shape[1]
    q = q.reshape(tokens, kv, -1, q.shape[-1])
    scores = jnp.einsum("tgsd,ugd->gstu", q.astype(jnp.float32), k.astype(jnp.float32)) * q.shape[-1] ** -0.5
    place = jnp.arange(tokens)
    weights = jax.nn.softmax(jnp.where(place[:, None] >= place, scores, -jnp.inf), -1).astype(jnp.bfloat16)
    return jnp.einsum("gstu,ugd->tgsd", weights.astype(jnp.float32), v.astype(jnp.float32)).astype(jnp.bfloat16).reshape(tokens, -1)


def layer(h, w):
    a = normed(h)
    q, k = (turned(matmul(a, w[name]).reshape(h.shape[0], -1, HEAD), THETA) for name in ("wq", "wk"))
    h = h + matmul(seen_by(q, k, matmul(a, w["wv"]).reshape(h.shape[0], -1, HEAD)), w["wo"])
    b = normed(h)
    gate = jnp.dot(b, w["w_gate"], preferred_element_type=jnp.float32)
    up = jnp.dot(b, w["w_up"], preferred_element_type=jnp.float32)
    return h + matmul((jax.nn.silu(gate) * up).astype(jnp.bfloat16), w["w_down"])


def adamw(w, m, v, g):
    m = 0.9 * m + 0.1 * g
    v = 0.95 * v + 0.05 * g * g
    step = m * lax.rsqrt(v + 1e-8) + 0.1 * w
    return (w - 0.02 * step).astype(jnp.bfloat16), m, v


def stack(weights, h):
    return lax.scan(lambda h, w: (layer(h, w), None), h, weights)[0]


def reference(x, dy, wq, wk, wv, wo, w_gate, w_up, w_down, m_wq, m_wk, m_wv, m_wo, m_w_gate, m_w_up, m_w_down, v_wq, v_wk, v_wv, v_wo, v_w_gate, v_w_up, v_w_down):
    weights = dict(zip(NAMES, (wq, wk, wv, wo, w_gate, w_up, w_down), strict=True))

    def take(so_far, sequence):
        h, by_y = sequence
        _, back = jax.vjp(stack, weights, h)
        by_weights, by_h = back(by_y)
        return jax.tree.map(lambda total, term: total + term.astype(jnp.float32), so_far, by_weights), by_h

    none_yet = {name: jnp.zeros(w.shape, jnp.float32) for name, w in weights.items()}
    by_weights, by_x = lax.scan(take, none_yet, (x, dy))
    gradients = [by_weights[name].astype(jnp.bfloat16).astype(jnp.float32) for name in NAMES]
    first = (m_wq, m_wk, m_wv, m_wo, m_w_gate, m_w_up, m_w_down)
    second = (v_wq, v_wk, v_wv, v_wo, v_w_gate, v_w_up, v_w_down)
    new = [adamw(weights[name].astype(jnp.float32), m, v, g) for name, m, v, g in zip(NAMES, first, second, gradients, strict=True)]
    return tuple(one[which] for which in range(3) for one in new)
```

```python
import functools

import jax
import jax.numpy as jnp
from jax import lax
from jax.experimental import pallas as pl
from jax.experimental.pallas import tpu as pltpu
from jax.sharding import PartitionSpec as P

LOG2E = 1.4426950408889634
VMEM = 63 * 2**20


def _fit(size, want, unit=128):
    return max(n for n in range(unit, max(min(want, size), unit) + 1, unit) if size % n == 0)


def _dot(a, b, ca, cb):
    return lax.dot_general(a, b, (((ca,), (cb,)), ((), ())), preferred_element_type=jnp.float32)


HEAD = 256
THETA = 10000
NAMES = ("wq", "wk", "wv", "wo", "w_gate", "w_up", "w_down")
BF, F32 = jnp.bfloat16, jnp.float32


def _params(*kinds):
    return pltpu.CompilerParams(dimension_semantics=kinds, vmem_limit_bytes=VMEM)


def _nn(a, b):
    return _dot(a, b, 1, 0)


def _nt(a, b):
    return _dot(a, b, 1, 1)


def _normed(h):
    wide = h.astype(F32)
    scale = lax.rsqrt(jnp.mean(wide * wide, -1, keepdims=True) + 1e-6)
    return wide * scale, scale


def _norm_back(y, scale, dy):
    return (scale * (dy - y * jnp.mean(dy * y, -1, keepdims=True))).astype(BF)


def tables(tokens):
    half, low = HEAD // 2, 64
    rate = THETA ** (-jnp.arange(half, dtype=F32) / half)
    far = (jnp.arange(tokens // low, dtype=F32) * low)[:, None, None] * rate
    near = jnp.arange(low, dtype=F32)[None, :, None] * rate
    ca, sa, cb, sb = jnp.cos(far), jnp.sin(far), jnp.cos(near), jnp.sin(near)
    return (ca * cb - sa * sb).reshape(tokens, half), (sa * cb + ca * sb).reshape(tokens, half)


def _turn(t, cos, sin):
    a, b = t[:, : HEAD // 2], t[:, HEAD // 2 :]
    return jnp.concatenate([a * cos - b * sin, b * cos + a * sin], -1)


def _whole(a, buffers=None):
    return pl.BlockSpec(a.shape, lambda *_: (0,) * a.ndim, pipeline_mode=buffers and pl.Buffered(buffers))


def _layer(w, rows=None, cols=None):
    a, number = w
    shape = (None, rows or a.shape[1], cols or a.shape[2])
    return pl.BlockSpec(shape, lambda f: (number, f if rows else 0, f if cols else 0))


def _rows(a, block):
    return pl.BlockSpec((block, a.shape[1]), lambda i: (i, 0))


def _heads(heads, block):
    return pl.BlockSpec((heads, block, HEAD), lambda i: (0, i, 0))


def _project(h_ref, wq_ref, wk_ref, wv_ref, cos_ref, sin_ref, q_ref, k_ref, v_ref):
    a = _normed(h_ref[...])[0].astype(BF)
    cos, sin = cos_ref[...], sin_ref[...]
    for w_ref, out_ref in ((wq_ref, q_ref), (wk_ref, k_ref), (wv_ref, v_ref)):
        t = _nn(a, w_ref[...]).astype(BF)
        for n in range(out_ref.shape[0]):
            part = t[:, n * HEAD : (n + 1) * HEAD]
            out_ref[n] = part if out_ref is v_ref else _turn(part.astype(F32), cos, sin).astype(BF)


def project(h, wq, wk, wv, cos, sin):
    t, d = h.shape
    bt = _fit(t, 512)
    heads = wq[0].shape[2] // HEAD
    return pl.pallas_call(
        _project,
        grid=(t // bt,),
        in_specs=[_rows(h, bt), _layer(wq), _layer(wk), _layer(wv), _rows(cos, bt), _rows(sin, bt)],
        out_specs=[_heads(heads, bt)] * 3,
        out_shape=[jax.ShapeDtypeStruct((heads, t, HEAD), BF)] * 3,
        compiler_params=_params("arbitrary"),
        cost_estimate=pl.CostEstimate(flops=6 * t * d * d, transcendentals=t, bytes_accessed=14 * t * d),
        name="project",
    )(h, wq[0], wk[0], wv[0], cos, sin)


def _after(h_ref, o_ref, wo_ref):
    o = jnp.concatenate([o_ref[n] for n in range(o_ref.shape[0])], -1)
    return (h_ref[...].astype(F32) + _nn(o, wo_ref[...]).astype(BF).astype(F32)).astype(BF)


def _feed(h_ref, o_ref, wo_ref, wg_ref, wu_ref, wd_ref, out_ref):
    h = _after(h_ref, o_ref, wo_ref)
    b = _normed(h)[0].astype(BF)
    total = None
    step = _fit(wg_ref.shape[1], 512)
    for f in range(0, wg_ref.shape[1], step):
        gate, up = _nn(b, wg_ref[:, f : f + step]), _nn(b, wu_ref[:, f : f + step])
        act = (gate * jax.nn.sigmoid(gate) * up).astype(BF)
        term = _nn(act, wd_ref[f : f + step, :])
        total = term if total is None else total + term
    out_ref[...] = (h.astype(F32) + total.astype(BF).astype(F32)).astype(BF)


def feed(h, o, wo, wg, wu, wd):
    t, d = h.shape
    bt = _fit(t, 512)
    return pl.pallas_call(
        _feed,
        grid=(t // bt,),
        in_specs=[_rows(h, bt), _heads(o.shape[0], bt), _layer(wo), _layer(wg), _layer(wu), _layer(wd)],
        out_specs=_rows(h, bt),
        out_shape=jax.ShapeDtypeStruct((t, d), BF),
        compiler_params=_params("arbitrary"),
        cost_estimate=pl.CostEstimate(flops=6 * t * d * wg[0].shape[2] + 2 * t * d * d, transcendentals=t * wg[0].shape[2], bytes_accessed=20 * t * d),
        name="feed",
    )(h, o, wo[0], wg[0], wu[0], wd[0])


def _feed_back(plan, h_ref, o_ref, dh_ref, wo_ref, wg_ref, wu_ref, wd_ref, *refs):
    if plan is not None:
        n, m = len(plan.ins), len(plan.pieces)
        plan.bind(refs[:n], refs[n + 7 : n + 7 + m], refs[n + m + 12 :])
        refs = refs[n : n + 7] + refs[n + 7 + m : n + m + 12]
    dh1_ref, do_ref, delta_ref, dwo_ref, dwg_ref, dwu_ref, dwd_ref, h1_s, b_s, bt_s, dt_s, db_s = refs
    f, last = pl.program_id(0), pl.num_programs(0) - 1
    t, d = h_ref.shape
    heads = o_ref.shape[0]
    block = _fit(t, 256)

    @pl.when(f == 0)
    def _():
        if plan is not None:
            plan.begin()

        def one(i, _):
            at = pl.ds(pl.multiple_of(i * block, block), block)
            o = jnp.concatenate([o_ref[n, at, :] for n in range(heads)], -1)
            h1 = (h_ref[at, :].astype(F32) + _nn(o, wo_ref[...]).astype(BF).astype(F32)).astype(BF)
            b = _normed(h1)[0].astype(BF)
            h1_s[at, :] = h1
            b_s[at, :] = b
            bt_s[:, at] = b.T
            dt_s[:, at] = dh_ref[at, :].T

        lax.fori_loop(0, t // block, one, None)
        if plan is not None:
            plan.share()

    wg, wu, wd = wg_ref[...], wu_ref[...], wd_ref[...]
    sums = [0.0, 0.0, 0.0]

    def first(at):
        b, dh = b_s[at : at + part, :], dh_ref[at : at + part, :]
        return _nn(b, wg), _nn(b, wu), _nt(dh, wd)

    def second(at, made):
        gate, up, dact = made
        dact = dact.astype(BF).astype(F32)
        sig = jax.nn.sigmoid(gate)
        s = gate * sig
        act, dup = (s * up).astype(BF), (dact * s).astype(BF)
        dgate = (dact * up * (sig + s * (1 - sig))).astype(BF)
        db = _nt(dgate, wg) + _nt(dup, wu)
        db_s[at : at + part, :] = jnp.where(f == 0, db, db_s[at : at + part, :] + db)
        for n, (left, right) in enumerate(((bt_s, dgate), (bt_s, dup), (dt_s, act))):
            sums[n] += _nn(left[:, at : at + part], right)

    part = _fit(t, 512)
    _staged([(at,) for at in range(0, t, part)], first, second)
    dwg_ref[...] = sums[0].astype(BF)
    dwu_ref[...] = sums[1].astype(BF)
    dwd_ref[...] = sums[2].astype(BF).T
    if plan is not None:
        plan.step(f)

    @pl.when(f == last)
    def _():
        def one(i, _):
            at = pl.ds(pl.multiple_of(i * block, block), block)
            y, scale = _normed(h1_s[at, :])
            back = _norm_back(y, scale, db_s[at, :].astype(BF).astype(F32))
            dh1 = (dh_ref[at, :].astype(F32) + back.astype(F32)).astype(BF)
            dh1_ref[at, :] = dh1
            do = _nt(dh1, wo_ref[...]).astype(BF)
            for n in range(heads):
                o, mine = o_ref[n, at, :], do[:, n * HEAD : (n + 1) * HEAD]
                do_ref[n, at, :] = mine
                delta_ref[n : n + 1, at] = (o.astype(F32) * mine.astype(F32)).T.sum(0, keepdims=True)

        lax.fori_loop(0, t // block, one, None)
        for n in range(heads):
            dwo_ref[n * HEAD : (n + 1) * HEAD, :] = _nn(o_ref[n].T, dh1_ref[...]).astype(BF)
        if plan is not None:
            plan.end()


def feed_back(h, o, dh, wo, wg, wu, wd, plan=None, collective_id=None):
    t, d = h.shape
    heads, ff = o.shape[0], wg[0].shape[2]
    bf = _fit(ff, 256)
    cols = pl.BlockSpec((d, bf), lambda f: (0, f))
    down = pl.BlockSpec((bf, d), lambda f: (f, 0))
    stats = jax.ShapeDtypeStruct((heads, t), F32)
    dwo, dwg, dwu, dwd = (jax.ShapeDtypeStruct(w[0].shape[1:], BF) for w in (wo, wg, wu, wd))
    ins, in_specs, out_specs, out_shape, scratch = (
        ([], [], [], [], []) if plan is None else (plan.ins, plan.in_specs, plan.out_specs, plan.out_shape, plan.scratch))
    params = {} if plan is None else dict(collective_id=collective_id, has_side_effects=True)
    return pl.pallas_call(
        functools.partial(_feed_back, plan),
        grid=(ff // bf,),
        in_specs=[_whole(h, 1), _whole(o, 1), _whole(dh, 1), _layer(wo), _layer(wg, cols=bf), _layer(wu, cols=bf), _layer(wd, rows=bf), *in_specs],
        out_specs=[_whole(h), _whole(o), _whole(stats), _whole(dwo), cols, cols, down, *out_specs],
        out_shape=[jax.ShapeDtypeStruct((t, d), BF), jax.ShapeDtypeStruct((heads, t, HEAD), BF), stats, dwo, dwg, dwu, dwd, *out_shape],
        scratch_shapes=[pltpu.VMEM((t, d), BF), pltpu.VMEM((t, d), BF), pltpu.VMEM((d, t), BF), pltpu.VMEM((d, t), BF), pltpu.VMEM((t, d), F32), *scratch],
        compiler_params=pltpu.CompilerParams(dimension_semantics=("arbitrary",), vmem_limit_bytes=VMEM, **params),
        cost_estimate=pl.CostEstimate(flops=16 * t * d * ff + 6 * t * d * d, transcendentals=t * ff, bytes_accessed=30 * t * d),
        name="feed_back" if plan is None else "feed_back_scatter",
    )(h, o, dh, wo[0], wg[0], wu[0], wd[0], *ins)


def _project_back(with_input, h_ref, dq_ref, dk_ref, dv_ref, cos_ref, sin_ref, *rest):
    if with_input:
        dh_ref, wq_ref, wk_ref, wv_ref, *rest, out_ref, tq, tk, tv = rest
        rest = [*rest, tq, tk, tv]
    dwq_ref, dwk_ref, dwv_ref, tq, tk, tv = rest
    i, last = pl.program_id(0), pl.num_programs(0) - 1
    y, scale = _normed(h_ref[...])
    at = y.astype(BF).T
    cos, sin = cos_ref[...], sin_ref[...]
    da = None
    for n, (g_ref, total, dw_ref) in enumerate(((dq_ref, tq, dwq_ref), (dk_ref, tk, dwk_ref), (dv_ref, tv, dwv_ref))):
        parts = [g_ref[m] for m in range(g_ref.shape[0])]
        if n < 2:
            parts = [_turn(p.astype(F32), cos, -sin).astype(BF) for p in parts]
        g = jnp.concatenate(parts, -1)
        term = _nn(at, g)
        total[...] = jnp.where(i == 0, term, total[...] + term)

        @pl.when(i == last)
        def _():
            dw_ref[...] = total[...].astype(BF)

        if with_input:
            back = _nt(g, (wq_ref, wk_ref, wv_ref)[n][...])
            da = back if da is None else da + back
    if with_input:
        back = _norm_back(y, scale, da.astype(BF).astype(F32))
        out_ref[...] = (dh_ref[...].astype(F32) + back.astype(F32)).astype(BF)


def project_back(h, dq, dk, dv, cos, sin, rest=None):
    t, d = h.shape
    bt = _fit(t, 512)
    heads = dq.shape[0]
    dw = jax.ShapeDtypeStruct((d, heads * HEAD), BF)
    more = [] if rest is None else [_rows(h, bt), *map(_layer, rest[1:])]
    return pl.pallas_call(
        functools.partial(_project_back, rest is not None),
        grid=(t // bt,),
        in_specs=[_rows(h, bt), *[_heads(heads, bt)] * 3, _rows(cos, bt), _rows(sin, bt), *more],
        out_specs=[_whole(dw)] * 3 + ([] if rest is None else [_rows(h, bt)]),
        out_shape=[dw] * 3 + ([] if rest is None else [jax.ShapeDtypeStruct((t, d), BF)]),
        scratch_shapes=[pltpu.VMEM(dw.shape, F32)] * 3,
        compiler_params=_params("arbitrary"),
        cost_estimate=pl.CostEstimate(flops=12 * t * d * d, transcendentals=t, bytes_accessed=16 * t * d),
        name="project_back",
    )(h, dq, dk, dv, cos, sin, *(() if rest is None else (rest[0], *(w[0] for w in rest[1:]))))


def adamw(w, m, v, g):
    m = 0.9 * m + 0.1 * g
    v = 0.95 * v + 0.05 * g * g
    step = m * lax.rsqrt(v + 1e-8) + 0.1 * w
    return (w - 0.02 * step).astype(jnp.bfloat16), m, v


def _strip(t):
    return _fit(t, 512)


def _staged(tasks, first, second):
    held = None
    for task in tasks:
        made = first(*task)
        if held is not None:
            second(*held)
        held = (*task, made)
    second(*held)


def _attend(q_ref, k_ref, v_ref, o_ref, lse_ref):
    heads, t, d = q_ref.shape
    e, bq = d**-0.5 * LOG2E, _strip(t)
    hidden = lax.broadcasted_iota(jnp.int32, (bq, bq), 0) < lax.broadcasted_iota(jnp.int32, (bq, bq), 1)

    def scores(h, at):
        q = q_ref[h, at : at + bq, :]
        own = jnp.where(hidden, -1e30, _nt(q, k_ref[h, at : at + bq, :]))
        return [own] + ([_nt(q, k_ref[h, :at, :])] if at else [])

    def mix(h, at, s):
        top = functools.reduce(jnp.maximum, [x.max(-1, keepdims=True) for x in s])
        p = [jnp.exp2((x - top) * e) for x in s]
        total = sum(x.sum(-1, keepdims=True) for x in p)
        out = _nn(p[0].astype(BF), v_ref[h, at : at + bq, :])
        if at:
            out += _nn(p[1].astype(BF), v_ref[h, :at, :])
        o_ref[h, at : at + bq, :] = (out * (1 / total)).astype(BF)
        lse = top * e + jnp.log2(total)
        lse_ref[h : h + 1, at : at + bq] = jnp.broadcast_to(lse, (bq, 128)).T[:1, :]

    _staged([(h, at) for at in range(0, t, bq) for h in range(heads)], scores, mix)


def attend(q, k, v):
    heads, t, d = q.shape
    vmem = pl.BlockSpec(memory_space=pltpu.VMEM)
    return pl.pallas_call(
        _attend,
        in_specs=[vmem] * 3,
        out_specs=[vmem] * 2,
        out_shape=[jax.ShapeDtypeStruct(q.shape, BF), jax.ShapeDtypeStruct((heads, t), F32)],
        compiler_params=_params(),
        cost_estimate=pl.CostEstimate(flops=2 * heads * t * t * d, transcendentals=heads * t * t // 2, bytes_accessed=8 * heads * t * d),
        name="attend",
    )(q, k, v)


def _attend_back(q_ref, k_ref, v_ref, do_ref, lse_ref, delta_ref, dq_ref, dk_ref, dv_ref, dq_s):
    heads, t, d = q_ref.shape
    scale, bk = d**-0.5, _strip(t)
    e = scale * LOG2E
    seen = lax.broadcasted_iota(jnp.int32, (bk, bk), 0) <= lax.broadcasted_iota(jnp.int32, (bk, bk), 1)

    def scores(h, at):
        return (_nt(k_ref[h, at : at + bk, :], q_ref[h, at:, :]), _nt(v_ref[h, at : at + bk, :], do_ref[h, at:, :]))

    def back(h, at, made):
        s, dp = made
        p = jnp.exp2(s * e - lse_ref[h : h + 1, at:])
        own = jnp.where(seen, p[:, :bk], 0.0)
        p = jnp.concatenate([own, p[:, bk:]], 1) if at + bk < t else own
        ds = (p * (dp - delta_ref[h : h + 1, at:])).astype(BF)
        dv_ref[h, at : at + bk, :] = _nn(p.astype(BF), do_ref[h, at:, :]).astype(BF)
        dk_ref[h, at : at + bk, :] = (_nn(ds, q_ref[h, at:, :]) * scale).astype(BF)
        dq = _nn(k_ref[h, at : at + bk, :].T, ds)
        if at:
            dq += dq_s[h, :, at:]
        dq_ref[h, at : at + bk, :] = (dq[:, :bk] * scale).T.astype(BF)
        if at + bk < t:
            dq_s[h, :, at + bk :] = dq[:, bk:]

    _staged([(h, at) for at in range(0, t, bk) for h in range(heads)], scores, back)


def attend_back(q, k, v, do, lse, delta):
    heads, t, d = q.shape
    vmem = pl.BlockSpec(memory_space=pltpu.VMEM)
    return pl.pallas_call(
        _attend_back,
        in_specs=[vmem] * 6,
        out_specs=[vmem] * 3,
        out_shape=[jax.ShapeDtypeStruct(q.shape, BF)] * 3,
        scratch_shapes=[pltpu.VMEM((heads, d, t), F32)],
        compiler_params=_params(),
        cost_estimate=pl.CostEstimate(flops=5 * heads * t * t * d, transcendentals=heads * t * t // 2, bytes_accessed=14 * heads * t * d),
        name="attend_back",
    )(q, k, v, do, lse, delta)


CHIPS = 8
MESH_ID = pl.DeviceIdType.MESH


def _place():
    me = lax.axis_index("dp")
    core, y, z = lax.rem(me, 2), lax.div(me, 8), lax.rem(lax.div(me, 2), 4)
    return z + y * (7 - 2 * z), core


def _member(place, core):
    at = lax.rem(place + 2 * CHIPS, CHIPS)
    y, r = lax.div(at, 4), lax.rem(at, 4)
    return (y * 4 + r + y * (3 - 2 * r)) * 2 + core


def _copy(src, dst, send, recv, member):
    return pltpu.make_async_remote_copy(src_ref=src, dst_ref=dst, send_sem=send, recv_sem=recv,
                                        device_id=(lax.axis_index("rep"), member), device_id_type=MESH_ID)


def _meet(members):
    barrier = pltpu.get_barrier_semaphore()
    for member in members:
        pl.semaphore_signal(barrier, inc=1, device_id=(lax.axis_index("rep"), member), device_id_type=MESH_ID)
    pl.semaphore_wait(barrier, len(members))


HOPS = 4


def _gather(late, *refs):
    n = len(late[0]) + len(late[1])
    own, out, (ring_send, ring_recv, pair_send, pair_recv, local) = refs[:n], refs[n : 2 * n], refs[2 * n :]
    place, core = _place()
    right, left, other = _member(place + 1, core), _member(place - 1, core), _member(place, 1 - core)

    def block(i, member):
        rows = own[i].shape[1]
        return out[i].at[:, pl.ds(pl.multiple_of(member * rows, rows), rows), :]

    def away(direction, hop):
        return _member(place - hop if direction == 0 else place + hop, core)

    def ring(direction, hop, i):
        dst = block(i, away(direction, hop - 1))
        return _copy(own[i] if hop == 1 else dst, dst, ring_send.at[direction, hop - 1, i], ring_recv.at[direction, hop - 1, i],
                     (right, left)[direction])

    def came(direction, hop, i):
        here = block(i, away(direction, hop))
        return _copy(here, here, ring_send.at[direction, hop - 1, i], ring_recv.at[direction, hop - 1, i], (right, left)[direction])

    def pair(slot, member, i, src=None):
        here = block(i, member)
        return _copy(here if src is None else src, here, pair_send.at[slot, i], pair_recv.at[slot, i], other)

    def goes(direction, hop, i):
        return hop < HOPS or i in late[direction]

    _meet((right, left, other))
    me = _member(place, core)
    mine = [pltpu.make_async_copy(own[i], block(i, me), local.at[i]) for i in range(n)]
    for i in range(n):
        for direction in range(2):
            ring(direction, 1, i).start()
        pair(0, me, i, own[i]).start()
        mine[i].start()
    for hop in range(1, HOPS + 1):
        for i in range(n):
            for direction in range(2):
                if goes(direction, hop, i):
                    came(direction, hop, i).wait_recv()
                    if hop < HOPS and goes(direction, hop + 1, i):
                        ring(direction, hop + 1, i).start()
                    pair(hop if direction == 0 or hop == HOPS else HOPS + hop, away(direction, hop), i).start()
    for i in range(n):
        mine[i].wait()
        for slot in range(CHIPS):
            hop = slot if slot <= HOPS else slot - HOPS
            direction = 1 if slot > HOPS or (slot == HOPS and i in late[1]) else 0
            far = _member(place - hop if direction == 0 else place + hop, 1 - core)
            here = block(i, far)
            _copy(here, here, pair_send.at[slot, i], pair_recv.at[slot, i], other).wait()
        for hop in range(1, HOPS + 1):
            for direction in range(2):
                if goes(direction, hop, i):
                    ring(direction, hop, i).wait_send()


def gather(weights, late, collective_id):
    n = len(weights)
    vmem, anywhere = pl.BlockSpec(memory_space=pltpu.VMEM), pl.BlockSpec(memory_space=pl.ANY)
    sems = pltpu.SemaphoreType.DMA
    return pl.pallas_call(
        functools.partial(_gather, late),
        in_specs=[vmem] * n,
        out_specs=[anywhere] * n,
        out_shape=[jax.ShapeDtypeStruct((w.shape[0], 2 * CHIPS * w.shape[1], w.shape[2]), w.dtype) for w in weights],
        scratch_shapes=[sems((2, HOPS, n)), sems((2, HOPS, n)), sems((CHIPS, n)), sems((CHIPS, n)), sems((n,))],
        compiler_params=pltpu.CompilerParams(collective_id=collective_id, has_side_effects=True, vmem_limit_bytes=VMEM),
        name="gather",
    )(*weights)


class Scatter:
    def __init__(self, layers):
        self.deep, n = range(len(layers)), len(NAMES)
        self.ins = []
        for g in layers:
            for i, x in enumerate(g):
                rows = x.shape[0] // (2 * CHIPS)
                self.ins.append(x.reshape((2 * CHIPS, rows, x.shape[1]) if i < n - 1 else (2 * CHIPS, 2, rows // 2, x.shape[1])))
        self.sources = [
            [[(n * l + i, None) for l in self.deep for i in (2 * d, 2 * d + 1)], [(n * l + 4 + d, None) for l in self.deep],
             [(n * l + 6, d) for l in self.deep]]
            for d in range(2)
        ]
        shapes = [(len(planes), *self.ins[planes[0][0]].shape[-2:]) for planes in self.sources[0]]
        self.pieces = [(d, k) for k in range(len(shapes)) for d in range(2)]
        m, sems = len(shapes), pltpu.SemaphoreType.DMA
        self.in_specs = [pl.BlockSpec(memory_space=pl.ANY)] * len(self.ins)
        self.out_specs = [pl.BlockSpec(memory_space=pltpu.VMEM)] * (2 * m)
        self.out_shape = [jax.ShapeDtypeStruct(shapes[k], BF) for _, k in self.pieces]
        self.scratch = [pltpu.VMEM((count, *shapes[k]), BF) for count in (2 * CHIPS, CHIPS, CHIPS - 1) for _, k in self.pieces]
        self.scratch += [sems((len(self.ins) + len(layers),)), *[sems((2, m, CHIPS))] * 2, *[sems((2, m, CHIPS - 1))] * 2]

    def results(self, out):
        got = dict(zip(self.pieces, out))
        return [[got[i // 2, 0][2 * l + i % 2] for i in range(4)] + [got[d, 1][l] for d in range(2)]
                + [jnp.concatenate([got[d, 2][l] for d in range(2)], 0)] for l in self.deep]


    def bind(self, ins, out, scratch):
        many = len(self.pieces)
        self.out, self.own, self.got, self.came = (
            dict(zip(self.pieces, refs)) for refs in (out, *(scratch[i * many : (i + 1) * many] for i in range(3))))
        load, self.pair_send, self.pair_recv, self.ring_send, self.ring_recv = scratch[3 * many :]
        self.place, self.core = _place()
        self.right, self.left = _member(self.place + 1, self.core), _member(self.place - 1, self.core)
        self.other = _member(self.place, 1 - self.core)
        self.loads = []
        for d, k in self.pieces:
            for plane, (i, half) in enumerate(self.sources[d][k]):
                src = ins[i] if half is None else ins[i].at[:, half]
                self.loads.append(((d, k), pltpu.make_async_copy(src, self.own[d, k].at[:, plane], load.at[len(self.loads)])))
        return self

    def begin(self):
        for _, copy in self.loads:
            copy.start()
        _meet((self.right, self.left, self.other))

    def share(self):
        for d, k in self.pieces:
            for key, copy in self.loads:
                if key == (d, k):
                    copy.wait()
            for s in range(CHIPS):
                self._pair(d, k, s).start()

    def _toward(self, d, s, core):
        return _member(self.place - 1 - s if d == 0 else self.place + 1 + s, core)

    def _pair(self, d, k, s):
        return _copy(self.own[d, k].at[self._toward(d, s, 1 - self.core)], self.got[d, k].at[s], self.pair_send.at[d, k, s],
                     self.pair_recv.at[d, k, s], self.other)

    def _ring(self, d, k, s):
        return _copy(self.got[d, k].at[s], self.came[d, k].at[s], self.ring_send.at[d, k, s], self.ring_recv.at[d, k, s],
                     (self.right, self.left)[d])

    def step(self, s):
        for d, k in self.pieces:
            own, got = self.own[d, k], self.got[d, k]
            self._pair(d, k, s).wait_recv()

            @pl.when(s == 0)
            def _():
                got[0] = (own[self._toward(d, 0, self.core)].astype(F32) + got[0].astype(F32)).astype(BF)
                self._ring(d, k, 0).start()

            @pl.when(s > 0)
            def _():
                self._ring(d, k, s - 1).wait_recv()
                total = own[self._toward(d, s, self.core)].astype(F32) + got[s].astype(F32) + self.came[d, k][s - 1].astype(F32)

                @pl.when(s < CHIPS - 1)
                def _():
                    got[s] = total.astype(BF)
                    self._ring(d, k, s).start()

                @pl.when(s == CHIPS - 1)
                def _():
                    self.out[d, k][...] = total.astype(BF)

    def end(self):
        for d, k in self.pieces:
            for s in range(CHIPS):
                self._pair(d, k, s).wait_send()
                if s < CHIPS - 1:
                    self._ring(d, k, s).wait_send()


def _scatter(plan, *refs):
    n, m = len(plan.ins), len(plan.pieces)
    plan.bind(refs[:n], refs[n : n + m], refs[n + m :])
    plan.begin()
    plan.share()
    lax.fori_loop(0, CHIPS, lambda s, _: plan.step(s), None)
    plan.end()


def scatter(layers, collective_id):
    plan = Scatter(layers)
    res = pl.pallas_call(
        functools.partial(_scatter, plan),
        in_specs=plan.in_specs,
        out_specs=plan.out_specs,
        out_shape=plan.out_shape,
        scratch_shapes=plan.scratch,
        compiler_params=pltpu.CompilerParams(collective_id=collective_id, has_side_effects=True, vmem_limit_bytes=VMEM),
        name="scatter",
    )(*plan.ins)
    return plan.results(res)


def solution(mesh):
    def step(x, dy, *arrays):
        weights, m, v = (arrays[i : i + 7] for i in (0, 7, 14))
        layers = weights[0].shape[0]
        whole = gather(weights, ((4, 5), (0, 1, 2, 3, 6)), 0)
        h, kept = x[0], []
        cos, sin = tables(h.shape[0])
        for number in range(layers):
            wq, wk, wv, wo, wg, wu, wd = ((w, number) for w in whole)
            q, k, v_ = project(h, wq, wk, wv, cos, sin)
            o, lse = attend(q, k, v_)
            kept.append((h, q, k, v_, o, lse))
            if number < layers - 1:
                h = feed(h, o, wo, wg, wu, wd)
        by_h, terms, mine = dy[0], [None] * layers, [None] * layers
        for number in reversed(range(layers)):
            wq, wk, wv, wo, wg, wu, wd = ((w, number) for w in whole)
            h, q, k, v_, o, lse = kept[number]
            plan = Scatter([terms[number + 1]]) if number + 1 < layers else None
            by_h, do, delta, dwo, dwg, dwu, dwd, *got = feed_back(h, o, by_h, wo, wg, wu, wd, plan, 2 + number)
            if got:
                mine[number + 1] = plan.results(got)[0]
            dq, dk, dv = attend_back(q, k, v_, do, lse, delta)
            dwq, dwk, dwv, *by_h = project_back(h, dq, dk, dv, cos, sin, (by_h, wq, wk, wv) if number else None)
            by_h = by_h[0] if by_h else None
            terms[number] = (dwq, dwk, dwv, dwo, dwg, dwu, dwd)
        mine[0] = scatter(terms[:1], 1)[0]
        gradients = [jnp.stack([mine[number][i] for number in range(layers)]).astype(F32) for i in range(7)]
        new = [adamw(w.astype(F32), a, b, g) for w, a, b, g in zip(weights, m, v, gradients, strict=True)]
        return tuple(one[which] for which in range(3) for one in new)

    states, cut = P(("rep", "dp"), None, None), P(None, "dp", None)
    return jax.shard_map(
        step,
        mesh=mesh,
        in_specs=(states, states) + (cut,) * 21,
        out_specs=(P("rep", "dp", None),) * 21,
        check_vma=False,
    )
```

```python
import functools

import jax
import jax.numpy as jnp
from jax import lax
from jax.experimental import pallas as pl
from jax.experimental.pallas import tpu as pltpu
from jax.sharding import PartitionSpec as P

LOG2E = 1.4426950408889634
VMEM = 63 * 2**20


def _fit(size, want, unit=128):
    return max(n for n in range(unit, max(min(want, size), unit) + 1, unit) if size % n == 0)


def _dot(a, b, ca, cb):
    return lax.dot_general(a, b, (((ca,), (cb,)), ((), ())), preferred_element_type=jnp.float32)


HEAD = 256
THETA = 10000
NAMES = ("wq", "wk", "wv", "wo", "w_gate", "w_up", "w_down")
BF, F32 = jnp.bfloat16, jnp.float32


def _params(*kinds):
    return pltpu.CompilerParams(dimension_semantics=kinds, vmem_limit_bytes=VMEM)


def _nn(a, b):
    return _dot(a, b, 1, 0)


def _nt(a, b):
    return _dot(a, b, 1, 1)


def _normed(h):
    wide = h.astype(F32)
    scale = lax.rsqrt(jnp.mean(wide * wide, -1, keepdims=True) + 1e-6)
    return wide * scale, scale


def _norm_back(y, scale, dy):
    return (scale * (dy - y * jnp.mean(dy * y, -1, keepdims=True))).astype(BF)


def tables(tokens):
    half, low = HEAD // 2, 64
    rate = THETA ** (-jnp.arange(half, dtype=F32) / half)
    far = (jnp.arange(tokens // low, dtype=F32) * low)[:, None, None] * rate
    near = jnp.arange(low, dtype=F32)[None, :, None] * rate
    ca, sa, cb, sb = jnp.cos(far), jnp.sin(far), jnp.cos(near), jnp.sin(near)
    return (ca * cb - sa * sb).reshape(tokens, half), (sa * cb + ca * sb).reshape(tokens, half)


def _turn(t, cos, sin):
    a, b = t[:, : HEAD // 2], t[:, HEAD // 2 :]
    return jnp.concatenate([a * cos - b * sin, b * cos + a * sin], -1)


def _whole(a, buffers=None):
    return pl.BlockSpec(a.shape, lambda *_: (0,) * a.ndim, pipeline_mode=buffers and pl.Buffered(buffers))


def _layer(w, rows=None, cols=None):
    a, number = w
    shape = (None, rows or a.shape[1], cols or a.shape[2])
    return pl.BlockSpec(shape, lambda f: (number, f if rows else 0, f if cols else 0))


def _rows(a, block):
    return pl.BlockSpec((block, a.shape[1]), lambda i: (i, 0))


def _heads(heads, block):
    return pl.BlockSpec((heads, block, HEAD), lambda i: (0, i, 0))


def _feed_back(plan, h_ref, o_ref, dh_ref, wo_ref, wg_ref, wu_ref, wd_ref, *refs):
    if plan is not None:
        n, m = len(plan.ins), len(plan.pieces)
        plan.bind(refs[:n], refs[n + 7 : n + 7 + m], refs[n + m + 12 :])
        refs = refs[n : n + 7] + refs[n + 7 + m : n + m + 12]
    dh1_ref, do_ref, delta_ref, dwo_ref, dwg_ref, dwu_ref, dwd_ref, h1_s, b_s, bt_s, dt_s, db_s = refs
    f, last = pl.program_id(0), pl.num_programs(0) - 1
    t, d = h_ref.shape
    heads = o_ref.shape[0]
    block = _fit(t, 256)

    @pl.when(f == 0)
    def _():
        if plan is not None:
            plan.begin()

        def one(i, _):
            at = pl.ds(pl.multiple_of(i * block, block), block)
            o = jnp.concatenate([o_ref[n, at, :] for n in range(heads)], -1)
            h1 = (h_ref[at, :].astype(F32) + _nn(o, wo_ref[...]).astype(BF).astype(F32)).astype(BF)
            b = _normed(h1)[0].astype(BF)
            h1_s[at, :] = h1
            b_s[at, :] = b
            bt_s[:, at] = b.T
            dt_s[:, at] = dh_ref[at, :].T

        lax.fori_loop(0, t // block, one, None)
        if plan is not None:
            plan.share()

    wg, wu, wd = wg_ref[...], wu_ref[...], wd_ref[...]
    sums = [0.0, 0.0, 0.0]

    def first(at):
        b, dh = b_s[at : at + part, :], dh_ref[at : at + part, :]
        return _nn(b, wg), _nn(b, wu), _nt(dh, wd)

    def second(at, made):
        gate, up, dact = made
        dact = dact.astype(BF).astype(F32)
        sig = jax.nn.sigmoid(gate)
        s = gate * sig
        act, dup = (s * up).astype(BF), (dact * s).astype(BF)
        dgate = (dact * up * (sig + s * (1 - sig))).astype(BF)
        db = _nt(dgate, wg) + _nt(dup, wu)
        db_s[at : at + part, :] = jnp.where(f == 0, db, db_s[at : at + part, :] + db)
        for n, (left, right) in enumerate(((bt_s, dgate), (bt_s, dup), (dt_s, act))):
            sums[n] += _nn(left[:, at : at + part], right)

    part = _fit(t, 512)
    _staged([(at,) for at in range(0, t, part)], first, second)
    dwg_ref[...] = sums[0].astype(BF)
    dwu_ref[...] = sums[1].astype(BF)
    dwd_ref[...] = sums[2].astype(BF).T
    if plan is not None:
        plan.step(f)

    @pl.when(f == last)
    def _():
        def one(i, _):
            at = pl.ds(pl.multiple_of(i * block, block), block)
            y, scale = _normed(h1_s[at, :])
            back = _norm_back(y, scale, db_s[at, :].astype(BF).astype(F32))
            dh1 = (dh_ref[at, :].astype(F32) + back.astype(F32)).astype(BF)
            dh1_ref[at, :] = dh1
            do = _nt(dh1, wo_ref[...]).astype(BF)
            for n in range(heads):
                o, mine = o_ref[n, at, :], do[:, n * HEAD : (n + 1) * HEAD]
                do_ref[n, at, :] = mine
                delta_ref[n : n + 1, at] = (o.astype(F32) * mine.astype(F32)).T.sum(0, keepdims=True)

        lax.fori_loop(0, t // block, one, None)
        for n in range(heads):
            dwo_ref[n * HEAD : (n + 1) * HEAD, :] = _nn(o_ref[n].T, dh1_ref[...]).astype(BF)
        if plan is not None:
            plan.end()


def feed_back(h, o, dh, wo, wg, wu, wd, plan=None, collective_id=None):
    t, d = h.shape
    heads, ff = o.shape[0], wg[0].shape[2]
    bf = _fit(ff, 256)
    cols = pl.BlockSpec((d, bf), lambda f: (0, f))
    down = pl.BlockSpec((bf, d), lambda f: (f, 0))
    stats = jax.ShapeDtypeStruct((heads, t), F32)
    dwo, dwg, dwu, dwd = (jax.ShapeDtypeStruct(w[0].shape[1:], BF) for w in (wo, wg, wu, wd))
    ins, in_specs, out_specs, out_shape, scratch = (
        ([], [], [], [], []) if plan is None else (plan.ins, plan.in_specs, plan.out_specs, plan.out_shape, plan.scratch))
    params = {} if plan is None else dict(collective_id=collective_id, has_side_effects=True)
    return pl.pallas_call(
        functools.partial(_feed_back, plan),
        grid=(ff // bf,),
        in_specs=[_whole(h, 1), _whole(o, 1), _whole(dh, 1), _layer(wo), _layer(wg, cols=bf), _layer(wu, cols=bf), _layer(wd, rows=bf), *in_specs],
        out_specs=[_whole(h), _whole(o), _whole(stats), _whole(dwo), cols, cols, down, *out_specs],
        out_shape=[jax.ShapeDtypeStruct((t, d), BF), jax.ShapeDtypeStruct((heads, t, HEAD), BF), stats, dwo, dwg, dwu, dwd, *out_shape],
        scratch_shapes=[pltpu.VMEM((t, d), BF), pltpu.VMEM((t, d), BF), pltpu.VMEM((d, t), BF), pltpu.VMEM((d, t), BF), pltpu.VMEM((t, d), F32), *scratch],
        compiler_params=pltpu.CompilerParams(dimension_semantics=("arbitrary",), vmem_limit_bytes=VMEM, **params),
        cost_estimate=pl.CostEstimate(flops=16 * t * d * ff + 6 * t * d * d, transcendentals=t * ff, bytes_accessed=30 * t * d),
        name="feed_back" if plan is None else "feed_back_scatter",
    )(h, o, dh, wo[0], wg[0], wu[0], wd[0], *ins)


def _project_back(with_input, h_ref, dq_ref, dk_ref, dv_ref, cos_ref, sin_ref, *rest):
    if with_input:
        dh_ref, wq_ref, wk_ref, wv_ref, *rest, out_ref, tq, tk, tv = rest
        rest = [*rest, tq, tk, tv]
    dwq_ref, dwk_ref, dwv_ref, tq, tk, tv = rest
    i, last = pl.program_id(0), pl.num_programs(0) - 1
    y, scale = _normed(h_ref[...])
    at = y.astype(BF).T
    cos, sin = cos_ref[...], sin_ref[...]
    da = None
    for n, (g_ref, total, dw_ref) in enumerate(((dq_ref, tq, dwq_ref), (dk_ref, tk, dwk_ref), (dv_ref, tv, dwv_ref))):
        parts = [g_ref[m] for m in range(g_ref.shape[0])]
        if n < 2:
            parts = [_turn(p.astype(F32), cos, -sin).astype(BF) for p in parts]
        g = jnp.concatenate(parts, -1)
        term = _nn(at, g)
        total[...] = jnp.where(i == 0, term, total[...] + term)

        @pl.when(i == last)
        def _():
            dw_ref[...] = total[...].astype(BF)

        if with_input:
            back = _nt(g, (wq_ref, wk_ref, wv_ref)[n][...])
            da = back if da is None else da + back
    if with_input:
        back = _norm_back(y, scale, da.astype(BF).astype(F32))
        out_ref[...] = (dh_ref[...].astype(F32) + back.astype(F32)).astype(BF)


def project_back(h, dq, dk, dv, cos, sin, rest=None):
    t, d = h.shape
    bt = _fit(t, 512)
    heads = dq.shape[0]
    dw = jax.ShapeDtypeStruct((d, heads * HEAD), BF)
    more = [] if rest is None else [_rows(h, bt), *map(_layer, rest[1:])]
    return pl.pallas_call(
        functools.partial(_project_back, rest is not None),
        grid=(t // bt,),
        in_specs=[_rows(h, bt), *[_heads(heads, bt)] * 3, _rows(cos, bt), _rows(sin, bt), *more],
        out_specs=[_whole(dw)] * 3 + ([] if rest is None else [_rows(h, bt)]),
        out_shape=[dw] * 3 + ([] if rest is None else [jax.ShapeDtypeStruct((t, d), BF)]),
        scratch_shapes=[pltpu.VMEM(dw.shape, F32)] * 3,
        compiler_params=_params("arbitrary"),
        cost_estimate=pl.CostEstimate(flops=12 * t * d * d, transcendentals=t, bytes_accessed=16 * t * d),
        name="project_back",
    )(h, dq, dk, dv, cos, sin, *(() if rest is None else (rest[0], *(w[0] for w in rest[1:]))))


def adamw(w, m, v, g):
    m = 0.9 * m + 0.1 * g
    v = 0.95 * v + 0.05 * g * g
    step = m * lax.rsqrt(v + 1e-8) + 0.1 * w
    return (w - 0.02 * step).astype(jnp.bfloat16), m, v


def _strip(t):
    return _fit(t, 512)


def _staged(tasks, first, second, after=lambda: None):
    held = None
    for task in tasks:
        made = first(*task)
        if held is not None:
            second(*held)
            after()
        held = (*task, made)
    second(*held)
    after()


def _attend(q_ref, k_ref, v_ref, o_ref, lse_ref, after=lambda: None):
    heads, t, d = q_ref.shape
    e, bq = d**-0.5 * LOG2E, _strip(t)
    hidden = lax.broadcasted_iota(jnp.int32, (bq, bq), 0) < lax.broadcasted_iota(jnp.int32, (bq, bq), 1)

    def scores(h, at):
        q = q_ref[h, at : at + bq, :]
        own = jnp.where(hidden, -1e30, _nt(q, k_ref[h, at : at + bq, :]))
        return [own] + ([_nt(q, k_ref[h, :at, :])] if at else [])

    def mix(h, at, s):
        top = functools.reduce(jnp.maximum, [x.max(-1, keepdims=True) for x in s])
        p = [jnp.exp2((x - top) * e) for x in s]
        total = sum(x.sum(-1, keepdims=True) for x in p)
        out = _nn(p[0].astype(BF), v_ref[h, at : at + bq, :])
        if at:
            out += _nn(p[1].astype(BF), v_ref[h, :at, :])
        o_ref[h, at : at + bq, :] = (out * (1 / total)).astype(BF)
        lse = top * e + jnp.log2(total)
        lse_ref[h : h + 1, at : at + bq] = jnp.broadcast_to(lse, (bq, 128)).T[:1, :]

    _staged([(h, at) for at in range(0, t, bq) for h in range(heads)], scores, mix, after)


def _attend_back(q_ref, k_ref, v_ref, do_ref, lse_ref, delta_ref, dq_ref, dk_ref, dv_ref, dq_s):
    heads, t, d = q_ref.shape
    scale, bk = d**-0.5, _strip(t)
    e = scale * LOG2E
    seen = lax.broadcasted_iota(jnp.int32, (bk, bk), 0) <= lax.broadcasted_iota(jnp.int32, (bk, bk), 1)

    def scores(h, at):
        return (_nt(k_ref[h, at : at + bk, :], q_ref[h, at:, :]), _nt(v_ref[h, at : at + bk, :], do_ref[h, at:, :]))

    def back(h, at, made):
        s, dp = made
        p = jnp.exp2(s * e - lse_ref[h : h + 1, at:])
        own = jnp.where(seen, p[:, :bk], 0.0)
        p = jnp.concatenate([own, p[:, bk:]], 1) if at + bk < t else own
        ds = (p * (dp - delta_ref[h : h + 1, at:])).astype(BF)
        dv_ref[h, at : at + bk, :] = _nn(p.astype(BF), do_ref[h, at:, :]).astype(BF)
        dk_ref[h, at : at + bk, :] = (_nn(ds, q_ref[h, at:, :]) * scale).astype(BF)
        dq = _nn(k_ref[h, at : at + bk, :].T, ds)
        if at:
            dq += dq_s[h, :, at:]
        dq_ref[h, at : at + bk, :] = (dq[:, :bk] * scale).T.astype(BF)
        if at + bk < t:
            dq_s[h, :, at + bk :] = dq[:, bk:]

    _staged([(h, at) for at in range(0, t, bk) for h in range(heads)], scores, back)


def attend_back(q, k, v, do, lse, delta):
    heads, t, d = q.shape
    vmem = pl.BlockSpec(memory_space=pltpu.VMEM)
    return pl.pallas_call(
        _attend_back,
        in_specs=[vmem] * 6,
        out_specs=[vmem] * 3,
        out_shape=[jax.ShapeDtypeStruct(q.shape, BF)] * 3,
        scratch_shapes=[pltpu.VMEM((heads, d, t), F32)],
        compiler_params=_params(),
        cost_estimate=pl.CostEstimate(flops=5 * heads * t * t * d, transcendentals=heads * t * t // 2, bytes_accessed=14 * heads * t * d),
        name="attend_back",
    )(q, k, v, do, lse, delta)


CHIPS = 8
MESH_ID = pl.DeviceIdType.MESH


def _place():
    me = lax.axis_index("dp")
    core, y, z = lax.rem(me, 2), lax.div(me, 8), lax.rem(lax.div(me, 2), 4)
    return z + y * (7 - 2 * z), core


def _member(place, core):
    at = lax.rem(place + 2 * CHIPS, CHIPS)
    y, r = lax.div(at, 4), lax.rem(at, 4)
    return (y * 4 + r + y * (3 - 2 * r)) * 2 + core


def _copy(src, dst, send, recv, member):
    return pltpu.make_async_remote_copy(src_ref=src, dst_ref=dst, send_sem=send, recv_sem=recv,
                                        device_id=(lax.axis_index("rep"), member), device_id_type=MESH_ID)


def _meet(members):
    barrier = pltpu.get_barrier_semaphore()
    for member in members:
        pl.semaphore_signal(barrier, inc=1, device_id=(lax.axis_index("rep"), member), device_id_type=MESH_ID)
    pl.semaphore_wait(barrier, len(members))


class Scatter:
    def __init__(self, layers):
        self.deep, n = range(len(layers)), len(NAMES)
        self.ins = []
        for g in layers:
            for i, x in enumerate(g):
                rows = x.shape[0] // (2 * CHIPS)
                self.ins.append(x.reshape((2 * CHIPS, rows, x.shape[1]) if i < n - 1 else (2 * CHIPS, 2, rows // 2, x.shape[1])))
        self.sources = [
            [[(n * l + i, None) for l in self.deep for i in (2 * d, 2 * d + 1)], [(n * l + 4 + d, None) for l in self.deep],
             [(n * l + 6, d) for l in self.deep]]
            for d in range(2)
        ]
        shapes = [(len(planes), *self.ins[planes[0][0]].shape[-2:]) for planes in self.sources[0]]
        self.pieces = [(d, k) for k in range(len(shapes)) for d in range(2)]
        m, sems = len(shapes), pltpu.SemaphoreType.DMA
        self.in_specs = [pl.BlockSpec(memory_space=pl.ANY)] * len(self.ins)
        self.out_specs = [pl.BlockSpec(memory_space=pltpu.VMEM)] * (2 * m)
        self.out_shape = [jax.ShapeDtypeStruct(shapes[k], BF) for _, k in self.pieces]
        self.scratch = [pltpu.VMEM((count, *shapes[k]), BF) for count in (2 * CHIPS, CHIPS, CHIPS - 1) for _, k in self.pieces]
        self.scratch += [sems((len(self.ins) + len(layers),)), *[sems((2, m, CHIPS))] * 2, *[sems((2, m, CHIPS - 1))] * 2]

    def results(self, out):
        got = dict(zip(self.pieces, out))
        return [[got[i // 2, 0][2 * l + i % 2] for i in range(4)] + [got[d, 1][l] for d in range(2)]
                + [jnp.concatenate([got[d, 2][l] for d in range(2)], 0)] for l in self.deep]


    def bind(self, ins, out, scratch):
        many = len(self.pieces)
        self.out, self.own, self.got, self.came = (
            dict(zip(self.pieces, refs)) for refs in (out, *(scratch[i * many : (i + 1) * many] for i in range(3))))
        load, self.pair_send, self.pair_recv, self.ring_send, self.ring_recv = scratch[3 * many :]
        self.place, self.core = _place()
        self.right, self.left = _member(self.place + 1, self.core), _member(self.place - 1, self.core)
        self.other = _member(self.place, 1 - self.core)
        self.loads = []
        for d, k in self.pieces:
            for plane, (i, half) in enumerate(self.sources[d][k]):
                src = ins[i] if half is None else ins[i].at[:, half]
                self.loads.append(((d, k), pltpu.make_async_copy(src, self.own[d, k].at[:, plane], load.at[len(self.loads)])))
        return self

    def begin(self):
        for _, copy in self.loads:
            copy.start()
        _meet((self.right, self.left, self.other))

    def share(self):
        for d, k in self.pieces:
            for key, copy in self.loads:
                if key == (d, k):
                    copy.wait()
            for s in range(CHIPS):
                self._pair(d, k, s).start()

    def _toward(self, d, s, core):
        return _member(self.place - 1 - s if d == 0 else self.place + 1 + s, core)

    def _pair(self, d, k, s):
        return _copy(self.own[d, k].at[self._toward(d, s, 1 - self.core)], self.got[d, k].at[s], self.pair_send.at[d, k, s],
                     self.pair_recv.at[d, k, s], self.other)

    def _ring(self, d, k, s):
        return _copy(self.got[d, k].at[s], self.came[d, k].at[s], self.ring_send.at[d, k, s], self.ring_recv.at[d, k, s],
                     (self.right, self.left)[d])

    def step(self, s):
        for d, k in self.pieces:
            own, got = self.own[d, k], self.got[d, k]
            self._pair(d, k, s).wait_recv()

            @pl.when(s == 0)
            def _():
                got[0] = (own[self._toward(d, 0, self.core)].astype(F32) + got[0].astype(F32)).astype(BF)
                self._ring(d, k, 0).start()

            @pl.when(s > 0)
            def _():
                self._ring(d, k, s - 1).wait_recv()
                total = own[self._toward(d, s, self.core)].astype(F32) + got[s].astype(F32) + self.came[d, k][s - 1].astype(F32)

                @pl.when(s < CHIPS - 1)
                def _():
                    got[s] = total.astype(BF)
                    self._ring(d, k, s).start()

                @pl.when(s == CHIPS - 1)
                def _():
                    self.out[d, k][...] = total.astype(BF)

    def end(self):
        for d, k in self.pieces:
            for s in range(CHIPS):
                self._pair(d, k, s).wait_send()
                if s < CHIPS - 1:
                    self._ring(d, k, s).wait_send()


def _scatter(plan, *refs):
    n, m = len(plan.ins), len(plan.pieces)
    plan.bind(refs[:n], refs[n : n + m], refs[n + m :])
    plan.begin()
    plan.share()
    lax.fori_loop(0, CHIPS, lambda s, _: plan.step(s), None)
    plan.end()


def scatter(layers, collective_id):
    plan = Scatter(layers)
    res = pl.pallas_call(
        functools.partial(_scatter, plan),
        in_specs=plan.in_specs,
        out_specs=plan.out_specs,
        out_shape=plan.out_shape,
        scratch_shapes=plan.scratch,
        compiler_params=pltpu.CompilerParams(collective_id=collective_id, has_side_effects=True, vmem_limit_bytes=VMEM),
        name="scatter",
    )(*plan.ins)
    return plan.results(res)


HOPS = 4
LATE = ((0, 4, 6), (1, 2, 3, 5))
RATE, DELAY = 46e3, 3.2


def _plan(sizes, groups, pieces):
    order = [i for items, _ in groups for i in items]
    due = {i: at for items, at in groups for i in items}
    busy, flying, unsent, now = [0.0, 0.0], [], list(order), 0.0
    slots = [[] for _ in range(len(pieces) + 1)]

    def put(hop, i, d):
        busy[d] = max(busy[d], now) + sizes[i] / RATE
        flying.append((busy[d] + DELAY, hop, i, d))

    def handle(slot, ready):
        for event in ready:
            flying.remove(event)
            _, hop, i, d = event
            slots[slot].append(("pass", hop, i, d))
            if hop + 1 < HOPS or (hop + 1 == HOPS and i % len(NAMES) in LATE[d]):
                put(hop + 1, i, d)

    def feed_links(slot, until):
        while unsent and min(busy) < until:
            i = unsent.pop(0)
            slots[slot].append(("send", i))
            put(1, i, 0)
            put(1, i, 1)

    rank = {i: n for n, i in enumerate(order)}
    for at in range(len(pieces) + 1):
        until = now + (pieces[at] if at < len(pieces) else 0.0)
        while True:
            handle(at, sorted((e for e in flying if e[0] <= now), key=lambda e: (due[e[2]], e[1], rank[e[2]], e[3])))
            feed_links(at, now + DELAY if any(due[i] <= at for i in order if i in unsent or any(e[2] == i for e in flying)) else until + 1)
            needed = [e for e in flying if due[e[2]] <= at or at == len(pieces)]
            if not needed and not (unsent and (due[unsent[0]] <= at or at == len(pieces))):
                break
            if needed:
                now = max(now, min(e[0] for e in (flying if at == len(pieces) else needed)))
            else:
                now += 0.5
        now += pieces[at] if at < len(pieces) else 0.0
    return slots, now


class Gather:
    def __init__(self, own, out, scratch, slots):
        self.own, self.out, self.slots = own, out, slots
        self.ring_send, self.ring_recv, self.pair_send, self.pair_recv, self.local, self.load = scratch
        self.place, self.core = _place()
        self.right, self.left = _member(self.place + 1, self.core), _member(self.place - 1, self.core)
        self.other = _member(self.place, 1 - self.core)
        self.at = 0

    def _block(self, i, member):
        layer, n = divmod(i, len(NAMES))
        rows = self.own[n].shape[1]
        return self.out[n].at[layer, pl.ds(pl.multiple_of(member * rows, rows), rows), :]

    def _away(self, d, hop, core):
        return _member(self.place - hop if d == 0 else self.place + hop, core)

    def _mine(self, i):
        layer, n = divmod(i, len(NAMES))
        return self.own[n].at[layer]

    def _ring(self, d, hop, i):
        dst = self._block(i, self._away(d, hop - 1, self.core))
        return _copy(self._mine(i) if hop == 1 else dst, dst, self.ring_send.at[d, hop - 1, i], self.ring_recv.at[d, hop - 1, i],
                     (self.right, self.left)[d])

    def _came(self, d, hop, i):
        here = self._block(i, self._away(d, hop, self.core))
        return _copy(here, here, self.ring_send.at[d, hop - 1, i], self.ring_recv.at[d, hop - 1, i], (self.right, self.left)[d])

    def _pair(self, slot, i, d, hop, core):
        here = self._block(i, self._away(d, hop, core))
        return _copy(self._mine(i) if slot == 0 else here, here, self.pair_send.at[slot, i], self.pair_recv.at[slot, i], self.other)

    def _keep(self, i):
        return pltpu.make_async_copy(self._mine(i), self._block(i, self._away(0, 0, self.core)), self.local.at[i])

    def begin(self):
        _meet((self.right, self.left, self.other))

    def tick(self):
        for what, *args in self.slots[self.at]:
            if what == "send":
                i = args[0]
                for d in range(2):
                    self._ring(d, 1, i).start()
                self._pair(0, i, 0, 0, self.core).start()
                self._keep(i).start()
            else:
                hop, i, d = args
                self._came(d, hop, i).wait_recv()
                if hop + 1 < HOPS or (hop + 1 == HOPS and i % len(NAMES) in LATE[d]):
                    self._ring(d, hop + 1, i).start()
                self._pair(hop if d == 0 or hop == HOPS else HOPS + hop, i, d, hop, self.core).start()
        self.at += 1

    def _far(self, i):
        for slot in range(CHIPS):
            hop = slot if slot <= HOPS else slot - HOPS
            yield slot, int(slot > HOPS or (slot == HOPS and i % len(NAMES) in LATE[1])), hop

    def fetch(self, i, ref):
        self._whole(i)
        self._fetched(i, ref).start()

    def _whole(self, i):
        self._keep(i).wait()
        for slot, d, hop in self._far(i):
            self._pair(slot, i, d, hop, 1 - self.core).wait_recv()

    def _fetched(self, i, ref):
        layer, n = divmod(i, len(NAMES))
        return pltpu.make_async_copy(self.out[n].at[layer], ref, self.load.at[i])

    def here(self, i, ref):
        self._fetched(i, ref).wait()

    def end(self, rest):
        for i in rest:
            self._whole(i)
        for i in range(self.local.shape[0]):
            for slot, d, hop in self._far(i):
                self._pair(slot, i, d, hop, self.core).wait_send()
                if slot:
                    self._ring(d, hop, i).wait_send()


def _forward(slots, layers, heads, x_ref, cos_ref, sin_ref, *refs):
    n = len(NAMES)
    own, refs = refs[:n], refs[n:]
    whole, h_ref, refs = refs[:n], refs[n], refs[n + 1 :]
    kept, refs = [refs[5 * l : 5 * l + 5] for l in range(layers)], refs[5 * layers :]
    w, comm = refs[:n], Gather(own, whole, refs[n:], slots)
    t = x_ref.shape[0]
    rows = _strip(t)
    comm.begin()
    comm.tick()
    for l in range(layers):
        q_ref, k_ref, v_ref, o_ref, lse_ref = kept[l]
        src = x_ref if l == 0 else h_ref
        for i in range(3):
            comm.fetch(n * l + i, w[i])
        for i in range(3):
            comm.here(n * l + i, w[i])
        for at in range(0, t, rows):
            block = slice(at, at + rows)
            a = _normed(src[block, :])[0].astype(BF)
            cos, sin = cos_ref[block, :], sin_ref[block, :]
            for w_ref, out_ref in zip(w, (q_ref, k_ref, v_ref)):
                r = _nn(a, w_ref[...]).astype(BF)
                for m in range(heads):
                    part = r[:, m * HEAD : (m + 1) * HEAD]
                    out_ref[m, block, :] = part if out_ref is v_ref else _turn(part.astype(F32), cos, sin).astype(BF)
            comm.tick()
        _attend(q_ref, k_ref, v_ref, o_ref, lse_ref, comm.tick)
        if l == layers - 1:
            break
        for i in range(3, n):
            comm.fetch(n * l + i, w[i])
        for i in range(3, n):
            comm.here(n * l + i, w[i])
        for at in range(0, t, rows):
            block = slice(at, at + rows)
            o = jnp.concatenate([o_ref[m, block, :] for m in range(heads)], -1)
            h = (src[block, :].astype(F32) + _nn(o, w[3][...]).astype(BF).astype(F32)).astype(BF)
            b = _normed(h)[0].astype(BF)
            total, step = None, _fit(w[4].shape[1], 512)
            for f in range(0, w[4].shape[1], step):
                gate, up = _nn(b, w[4][:, f : f + step]), _nn(b, w[5][:, f : f + step])
                term = _nn((gate * jax.nn.sigmoid(gate) * up).astype(BF), w[6][f : f + step, :])
                total = term if total is None else total + term
            h_ref[block, :] = (h.astype(F32) + total.astype(BF).astype(F32)).astype(BF)
            comm.tick()
    comm.end([n * (layers - 1) + i for i in range(3, n)])


def forward(x, weights, cos, sin, collective_id):
    n, layers = len(NAMES), weights[0].shape[0]
    t, d = x.shape
    heads = weights[0].shape[2] // HEAD
    whole = [jax.ShapeDtypeStruct((w.shape[0], 2 * CHIPS * w.shape[1], w.shape[2]), BF) for w in weights]
    sizes = {l * n + i: weights[i][0].size * 2 for l in range(layers) for i in range(n)}
    blocks = t // _strip(t)
    project_us, attend_us, feed_us = [1.7] * blocks, [0.45 * (b + 1) for b in range(blocks) for _ in range(heads)], [4.6] * blocks
    pieces, groups = [], []
    for l in range(layers):
        groups.append((range(n * l, n * l + 3), len(pieces)))
        pieces += project_us + attend_us
        groups.append((range(n * l + 3, n * l + n), len(pieces)))
        pieces += feed_us if l < layers - 1 else []
    slots, _ = _plan(sizes, groups, pieces)
    vmem, anywhere, sems = pl.BlockSpec(memory_space=pltpu.VMEM), pl.BlockSpec(memory_space=pl.ANY), pltpu.SemaphoreType.DMA
    head = jax.ShapeDtypeStruct((heads, t, HEAD), BF)
    kept = [head, head, head, head, jax.ShapeDtypeStruct((heads, t), F32)]
    res = pl.pallas_call(
        functools.partial(_forward, slots, layers, heads),
        in_specs=[vmem] * (3 + n),
        out_specs=[anywhere] * n + [vmem] * (1 + 5 * layers),
        out_shape=[*whole, jax.ShapeDtypeStruct((t, d), BF), *kept * layers],
        scratch_shapes=[*[pltpu.VMEM(w.shape[1:], BF) for w in whole], *[sems((2, HOPS, n * layers))] * 2, *[sems((CHIPS, n * layers))] * 2,
                        *[sems((n * layers,))] * 2],
        compiler_params=pltpu.CompilerParams(collective_id=collective_id, has_side_effects=True, vmem_limit_bytes=VMEM),
        name="forward",
    )(x, cos, sin, *weights)
    return res[:n], [x, res[n]], [res[n + 1 + 5 * l : n + 6 + 5 * l] for l in range(layers)]


def solution(mesh):
    def step(x, dy, *arrays):
        weights, m, v = (arrays[i : i + 7] for i in (0, 7, 14))
        layers = weights[0].shape[0]
        cos, sin = tables(x.shape[1])
        whole, states, kept = forward(x[0], weights, cos, sin, 0)
        by_h, terms, mine = dy[0], [None] * layers, [None] * layers
        for number in reversed(range(layers)):
            wq, wk, wv, wo, wg, wu, wd = ((w, number) for w in whole)
            h, (q, k, v_, o, lse) = states[number], kept[number]
            plan = Scatter([terms[number + 1]]) if number + 1 < layers else None
            by_h, do, delta, dwo, dwg, dwu, dwd, *got = feed_back(h, o, by_h, wo, wg, wu, wd, plan, 2 + number)
            if got:
                mine[number + 1] = plan.results(got)[0]
            dq, dk, dv = attend_back(q, k, v_, do, lse, delta)
            dwq, dwk, dwv, *by_h = project_back(h, dq, dk, dv, cos, sin, (by_h, wq, wk, wv) if number else None)
            by_h = by_h[0] if by_h else None
            terms[number] = (dwq, dwk, dwv, dwo, dwg, dwu, dwd)
        mine[0] = scatter(terms[:1], 1)[0]
        gradients = [jnp.stack([mine[number][i] for number in range(layers)]).astype(F32) for i in range(7)]
        new = [adamw(w.astype(F32), a, b, g) for w, a, b, g in zip(weights, m, v, gradients, strict=True)]
        return tuple(one[which] for which in range(3) for one in new)

    rows, cut = P(("rep", "dp"), None, None), P(None, "dp", None)
    return jax.shard_map(
        step,
        mesh=mesh,
        in_specs=(rows, rows) + (cut,) * 21,
        out_specs=(P("rep", "dp", None),) * 21,
        check_vma=False,
    )
```

```python
import functools

import jax
import jax.numpy as jnp
from jax import lax
from jax.experimental import pallas as pl
from jax.experimental.pallas import tpu as pltpu
from jax.sharding import PartitionSpec as P

LOG2E = 1.4426950408889634
VMEM = 63 * 2**20


def _fit(size, want, unit=128):
    return max(n for n in range(unit, max(min(want, size), unit) + 1, unit) if size % n == 0)


def _dot(a, b, ca, cb):
    return lax.dot_general(a, b, (((ca,), (cb,)), ((), ())), preferred_element_type=jnp.float32)


HEAD = 256
THETA = 10000
NAMES = ("wq", "wk", "wv", "wo", "w_gate", "w_up", "w_down")
BF, F32 = jnp.bfloat16, jnp.float32


def _params(*kinds):
    return pltpu.CompilerParams(dimension_semantics=kinds, vmem_limit_bytes=VMEM)


def _nn(a, b):
    return _dot(a, b, 1, 0)


def _nt(a, b):
    return _dot(a, b, 1, 1)


def _normed(h):
    wide = h.astype(F32)
    scale = lax.rsqrt(jnp.mean(wide * wide, -1, keepdims=True) + 1e-6)
    return wide * scale, scale


def _norm_back(y, scale, dy):
    return (scale * (dy - y * jnp.mean(dy * y, -1, keepdims=True))).astype(BF)


def tables(tokens):
    half, low = HEAD // 2, 64
    rate = THETA ** (-jnp.arange(half, dtype=F32) / half)
    far = (jnp.arange(tokens // low, dtype=F32) * low)[:, None, None] * rate
    near = jnp.arange(low, dtype=F32)[None, :, None] * rate
    ca, sa, cb, sb = jnp.cos(far), jnp.sin(far), jnp.cos(near), jnp.sin(near)
    return (ca * cb - sa * sb).reshape(tokens, half), (sa * cb + ca * sb).reshape(tokens, half)


def _turn(t, cos, sin):
    a, b = t[:, : HEAD // 2], t[:, HEAD // 2 :]
    return jnp.concatenate([a * cos - b * sin, b * cos + a * sin], -1)


def _whole(a, buffers=None):
    return pl.BlockSpec(a.shape, lambda *_: (0,) * a.ndim, pipeline_mode=buffers and pl.Buffered(buffers))


def _layer(w, rows=None, cols=None):
    a, number = w
    shape = (None, rows or a.shape[1], cols or a.shape[2])
    return pl.BlockSpec(shape, lambda f: (number, f if rows else 0, f if cols else 0))


def _rows(a, block):
    return pl.BlockSpec((block, a.shape[1]), lambda i: (i, 0))


def _heads(heads, block):
    return pl.BlockSpec((heads, block, HEAD), lambda i: (0, i, 0))


def _feed_back(plan, h_ref, o_ref, dh_ref, wo_ref, wg_ref, wu_ref, wd_ref, *refs):
    if plan is not None:
        n, m = len(plan.ins), len(plan.pieces)
        plan.bind(refs[:n], refs[n + 7 : n + 7 + m], refs[n + m + 12 :])
        refs = refs[n : n + 7] + refs[n + 7 + m : n + m + 12]
    dh1_ref, do_ref, delta_ref, dwo_ref, dwg_ref, dwu_ref, dwd_ref, h1_s, b_s, bt_s, dt_s, db_s = refs
    f, last = pl.program_id(0), pl.num_programs(0) - 1
    t, d = h_ref.shape
    heads = o_ref.shape[0]
    block = _fit(t, 256)

    @pl.when(f == 0)
    def _():
        if plan is not None:
            plan.begin()

        def one(i, _):
            at = pl.ds(pl.multiple_of(i * block, block), block)
            o = jnp.concatenate([o_ref[n, at, :] for n in range(heads)], -1)
            h1 = (h_ref[at, :].astype(F32) + _nn(o, wo_ref[...]).astype(BF).astype(F32)).astype(BF)
            b = _normed(h1)[0].astype(BF)
            h1_s[at, :] = h1
            b_s[at, :] = b
            bt_s[:, at] = b.T
            dt_s[:, at] = dh_ref[at, :].T

        lax.fori_loop(0, t // block, one, None)
        if plan is not None:
            plan.share()

    wg, wu, wd = wg_ref[...], wu_ref[...], wd_ref[...]
    sums = [0.0, 0.0, 0.0]

    def first(at):
        b, dh = b_s[at : at + part, :], dh_ref[at : at + part, :]
        return _nn(b, wg), _nn(b, wu), _nt(dh, wd)

    def second(at, made):
        gate, up, dact = made
        dact = dact.astype(BF).astype(F32)
        sig = jax.nn.sigmoid(gate)
        s = gate * sig
        act, dup = (s * up).astype(BF), (dact * s).astype(BF)
        dgate = (dact * up * (sig + s * (1 - sig))).astype(BF)
        db = _nt(dgate, wg) + _nt(dup, wu)
        db_s[at : at + part, :] = jnp.where(f == 0, db, db_s[at : at + part, :] + db)
        for n, (left, right) in enumerate(((bt_s, dgate), (bt_s, dup), (dt_s, act))):
            sums[n] += _nn(left[:, at : at + part], right)

    part = _fit(t, 512)
    def after():
        done.append(None)
        if plan is not None and len(done) == t // part // 2:
            plan.step(f, (0, 2))

    done = []
    _staged([(at,) for at in range(0, t, part)], first, second, after)
    dwg_ref[...] = sums[0].astype(BF)
    dwu_ref[...] = sums[1].astype(BF)
    dwd_ref[...] = sums[2].astype(BF).T
    if plan is not None:
        plan.step(f, (1,))

    @pl.when(f == last)
    def _():
        def one(i, _):
            at = pl.ds(pl.multiple_of(i * block, block), block)
            y, scale = _normed(h1_s[at, :])
            back = _norm_back(y, scale, db_s[at, :].astype(BF).astype(F32))
            dh1 = (dh_ref[at, :].astype(F32) + back.astype(F32)).astype(BF)
            dh1_ref[at, :] = dh1
            do = _nt(dh1, wo_ref[...]).astype(BF)
            for n in range(heads):
                o, mine = o_ref[n, at, :], do[:, n * HEAD : (n + 1) * HEAD]
                do_ref[n, at, :] = mine
                delta_ref[n : n + 1, at] = (o.astype(F32) * mine.astype(F32)).T.sum(0, keepdims=True)

        lax.fori_loop(0, t // block, one, None)
        for n in range(heads):
            dwo_ref[n * HEAD : (n + 1) * HEAD, :] = _nn(o_ref[n].T, dh1_ref[...]).astype(BF)
        if plan is not None:
            plan.end()


def feed_back(h, o, dh, wo, wg, wu, wd, plan=None, collective_id=None):
    t, d = h.shape
    heads, ff = o.shape[0], wg[0].shape[2]
    bf = _fit(ff, 256)
    cols = pl.BlockSpec((d, bf), lambda f: (0, f))
    down = pl.BlockSpec((bf, d), lambda f: (f, 0))
    stats = jax.ShapeDtypeStruct((heads, t), F32)
    dwo, dwg, dwu, dwd = (jax.ShapeDtypeStruct(w[0].shape[1:], BF) for w in (wo, wg, wu, wd))
    ins, in_specs, out_specs, out_shape, scratch = (
        ([], [], [], [], []) if plan is None else (plan.ins, plan.in_specs, plan.out_specs, plan.out_shape, plan.scratch))
    params = {} if plan is None else dict(collective_id=collective_id, has_side_effects=True)
    return pl.pallas_call(
        functools.partial(_feed_back, plan),
        grid=(ff // bf,),
        in_specs=[_whole(h, 1), _whole(o, 1), _whole(dh, 1), _layer(wo), _layer(wg, cols=bf), _layer(wu, cols=bf), _layer(wd, rows=bf), *in_specs],
        out_specs=[_whole(h), _whole(o), _whole(stats), _whole(dwo), cols, cols, down, *out_specs],
        out_shape=[jax.ShapeDtypeStruct((t, d), BF), jax.ShapeDtypeStruct((heads, t, HEAD), BF), stats, dwo, dwg, dwu, dwd, *out_shape],
        scratch_shapes=[pltpu.VMEM((t, d), BF), pltpu.VMEM((t, d), BF), pltpu.VMEM((d, t), BF), pltpu.VMEM((d, t), BF), pltpu.VMEM((t, d), F32), *scratch],
        compiler_params=pltpu.CompilerParams(dimension_semantics=("arbitrary",), vmem_limit_bytes=VMEM, **params),
        cost_estimate=pl.CostEstimate(flops=16 * t * d * ff + 6 * t * d * d, transcendentals=t * ff, bytes_accessed=30 * t * d),
        name="feed_back" if plan is None else "feed_back_scatter",
    )(h, o, dh, wo[0], wg[0], wu[0], wd[0], *ins)


def adamw(w, m, v, g):
    m = 0.9 * m + 0.1 * g
    v = 0.95 * v + 0.05 * g * g
    step = m * lax.rsqrt(v + 1e-8) + 0.1 * w
    return (w - 0.02 * step).astype(jnp.bfloat16), m, v


def _strip(t):
    return _fit(t, 512)


def _staged(tasks, first, second, after=lambda: None):
    held = None
    for task in tasks:
        made = first(*task)
        if held is not None:
            second(*held)
            after()
        held = (*task, made)
    second(*held)
    after()


def _attend(q_ref, k_ref, v_ref, o_ref, lse_ref, after=lambda: None):
    heads, t, d = q_ref.shape
    e, bq = d**-0.5 * LOG2E, _strip(t)
    hidden = lax.broadcasted_iota(jnp.int32, (bq, bq), 0) < lax.broadcasted_iota(jnp.int32, (bq, bq), 1)

    def scores(h, at):
        q = q_ref[h, at : at + bq, :]
        own = jnp.where(hidden, -1e30, _nt(q, k_ref[h, at : at + bq, :]))
        return [own] + ([_nt(q, k_ref[h, :at, :])] if at else [])

    def mix(h, at, s):
        top = functools.reduce(jnp.maximum, [x.max(-1, keepdims=True) for x in s])
        p = [jnp.exp2((x - top) * e) for x in s]
        total = sum(x.sum(-1, keepdims=True) for x in p)
        out = _nn(p[0].astype(BF), v_ref[h, at : at + bq, :])
        if at:
            out += _nn(p[1].astype(BF), v_ref[h, :at, :])
        o_ref[h, at : at + bq, :] = (out * (1 / total)).astype(BF)
        lse = top * e + jnp.log2(total)
        lse_ref[h : h + 1, at : at + bq] = jnp.broadcast_to(lse, (bq, 128)).T[:1, :]

    _staged([(h, at) for at in range(0, t, bq) for h in range(heads)], scores, mix, after)


def _back(with_input, q_ref, k_ref, v_ref, do_ref, lse_ref, delta_ref, *refs):
    n = 7 if with_input else 3
    late, refs = refs[:n], refs[n:]
    dws, refs = refs[:3], refs[3:]
    out_ref, refs = (refs[0], refs[1:]) if with_input else (None, refs)
    dq_s, held, sems = refs[0], refs[1 : n + 1], refs[n + 1]
    copies = [pltpu.make_async_copy(src, dst, sems.at[i]) for i, (src, dst) in enumerate(zip(late, held))]
    for copy in copies:
        copy.start()
    h_ref, cos_ref, sin_ref, *more = held
    heads, t, d = q_ref.shape
    scale, bk = d**-0.5, _strip(t)
    e = scale * LOG2E
    seen = lax.broadcasted_iota(jnp.int32, (bk, bk), 0) <= lax.broadcasted_iota(jnp.int32, (bk, bk), 1)
    parts, sums = {}, [0.0, 0.0, 0.0]

    def scores(h, at):
        return (_nt(k_ref[h, at : at + bk, :], q_ref[h, at:, :]), _nt(v_ref[h, at : at + bk, :], do_ref[h, at:, :]))

    def back(h, at, made):
        s, dp = made
        p = jnp.exp2(s * e - lse_ref[h : h + 1, at:])
        own = jnp.where(seen, p[:, :bk], 0.0)
        p = jnp.concatenate([own, p[:, bk:]], 1) if at + bk < t else own
        ds = (p * (dp - delta_ref[h : h + 1, at:])).astype(BF)
        dv = _nn(p.astype(BF), do_ref[h, at:, :]).astype(BF)
        dk = (_nn(ds, q_ref[h, at:, :]) * scale).astype(BF)
        dq = _nn(k_ref[h, at : at + bk, :].T, ds)
        if at:
            dq += dq_s[h, :, at:]
        if at + bk < t:
            dq_s[h, :, at + bk :] = dq[:, bk:]
        parts[h] = ((dq[:, :bk] * scale).T.astype(BF), dk, dv)
        if h == heads - 1:
            project(slice(at, at + bk))

    def project(block):
        if block.start == 0:
            for copy in copies:
                copy.wait()
        y, norm = _normed(h_ref[block, :])
        left = y.astype(BF).T
        cos, sin = cos_ref[block, :], sin_ref[block, :]
        da = None
        for n in range(3):
            g = [parts[h][n] for h in range(heads)]
            if n < 2:
                g = [_turn(x.astype(F32), cos, -sin).astype(BF) for x in g]
            g = jnp.concatenate(g, -1)
            sums[n] += _nn(left, g)
            if with_input:
                term = _nt(g, more[1 + n][...])
                da = term if da is None else da + term
        if with_input:
            add = _norm_back(y, norm, da.astype(BF).astype(F32))
            out_ref[block, :] = (more[0][block, :].astype(F32) + add.astype(F32)).astype(BF)

    _staged([(h, at) for at in range(0, t, bk) for h in range(heads)], scores, back)
    for n in range(3):
        dws[n][...] = sums[n].astype(BF)


def attend_back(q, k, v, do, lse, delta, h, cos, sin, rest=None):
    heads, t, d = q.shape
    late = [h, cos, sin, *(rest or ())]
    dw = jax.ShapeDtypeStruct((h.shape[1], heads * HEAD), BF)
    vmem, anywhere = pl.BlockSpec(memory_space=pltpu.VMEM), pl.BlockSpec(memory_space=pl.ANY)
    more = [] if rest is None else [jax.ShapeDtypeStruct(h.shape, BF)]
    return pl.pallas_call(
        functools.partial(_back, rest is not None),
        in_specs=[vmem] * 6 + [anywhere] * len(late),
        out_specs=[vmem] * (3 + len(more)),
        out_shape=[dw] * 3 + more,
        scratch_shapes=[pltpu.VMEM((heads, d, t), F32), *[pltpu.VMEM(a.shape, a.dtype) for a in late], pltpu.SemaphoreType.DMA((len(late),))],
        compiler_params=_params(),
        cost_estimate=pl.CostEstimate(flops=5 * heads * t * t * d, transcendentals=heads * t * t // 2, bytes_accessed=24 * heads * t * d),
        name="attend_back",
    )(q, k, v, do, lse, delta, *late)


CHIPS = 8
MESH_ID = pl.DeviceIdType.MESH


def _place():
    me = lax.axis_index("dp")
    core, y, z = lax.rem(me, 2), lax.div(me, 8), lax.rem(lax.div(me, 2), 4)
    return z + y * (7 - 2 * z), core


def _member(place, core):
    at = lax.rem(place + 2 * CHIPS, CHIPS)
    y, r = lax.div(at, 4), lax.rem(at, 4)
    return (y * 4 + r + y * (3 - 2 * r)) * 2 + core


def _copy(src, dst, send, recv, member):
    return pltpu.make_async_remote_copy(src_ref=src, dst_ref=dst, send_sem=send, recv_sem=recv,
                                        device_id=(lax.axis_index("rep"), member), device_id_type=MESH_ID)


def _meet(members):
    barrier = pltpu.get_barrier_semaphore()
    for member in members:
        pl.semaphore_signal(barrier, inc=1, device_id=(lax.axis_index("rep"), member), device_id_type=MESH_ID)
    pl.semaphore_wait(barrier, len(members))


class Scatter:
    def __init__(self, layers):
        self.deep, n = range(len(layers)), len(NAMES)
        self.ins = []
        for g in layers:
            for i, x in enumerate(g):
                rows = x.shape[0] // (2 * CHIPS)
                self.ins.append(x.reshape((2 * CHIPS, rows, x.shape[1]) if i < n - 1 else (2 * CHIPS, 2, rows // 2, x.shape[1])))
        self.sources = [
            [[(n * l + i, None) for l in self.deep for i in (2 * d, 2 * d + 1)], [(n * l + 4 + d, None) for l in self.deep],
             [(n * l + 6, d) for l in self.deep]]
            for d in range(2)
        ]
        shapes = [(len(planes), *self.ins[planes[0][0]].shape[-2:]) for planes in self.sources[0]]
        self.pieces = [(d, k) for k in range(len(shapes)) for d in range(2)]
        m, sems = len(shapes), pltpu.SemaphoreType.DMA
        self.in_specs = [pl.BlockSpec(memory_space=pl.ANY)] * len(self.ins)
        self.out_specs = [pl.BlockSpec(memory_space=pltpu.VMEM)] * (2 * m)
        self.out_shape = [jax.ShapeDtypeStruct(shapes[k], BF) for _, k in self.pieces]
        self.scratch = [pltpu.VMEM((count, *shapes[k]), BF) for count in (2 * CHIPS, CHIPS, CHIPS - 1) for _, k in self.pieces]
        self.scratch += [sems((len(self.ins) + len(layers),)), *[sems((2, m, CHIPS))] * 2, *[sems((2, m, CHIPS - 1))] * 2]

    def results(self, out):
        got = dict(zip(self.pieces, out))
        return [[got[i // 2, 0][2 * l + i % 2] for i in range(4)] + [got[d, 1][l] for d in range(2)]
                + [jnp.concatenate([got[d, 2][l] for d in range(2)], 0)] for l in self.deep]


    def bind(self, ins, out, scratch):
        many = len(self.pieces)
        self.out, self.own, self.got, self.came = (
            dict(zip(self.pieces, refs)) for refs in (out, *(scratch[i * many : (i + 1) * many] for i in range(3))))
        load, self.pair_send, self.pair_recv, self.ring_send, self.ring_recv = scratch[3 * many :]
        self.place, self.core = _place()
        self.right, self.left = _member(self.place + 1, self.core), _member(self.place - 1, self.core)
        self.other = _member(self.place, 1 - self.core)
        self.loads = []
        for d, k in self.pieces:
            for plane, (i, half) in enumerate(self.sources[d][k]):
                src = ins[i] if half is None else ins[i].at[:, half]
                self.loads.append(((d, k), pltpu.make_async_copy(src, self.own[d, k].at[:, plane], load.at[len(self.loads)])))
        return self

    def begin(self):
        for _, copy in self.loads:
            copy.start()
        _meet((self.right, self.left, self.other))

    def share(self):
        for d, k in sorted(self.pieces, key=lambda p: p[1] == 1):
            for key, copy in self.loads:
                if key == (d, k):
                    copy.wait()
            for s in range(CHIPS):
                self._pair(d, k, s).start()

    def _toward(self, d, s, core):
        return _member(self.place - 1 - s if d == 0 else self.place + 1 + s, core)

    def _pair(self, d, k, s):
        return _copy(self.own[d, k].at[self._toward(d, s, 1 - self.core)], self.got[d, k].at[s], self.pair_send.at[d, k, s],
                     self.pair_recv.at[d, k, s], self.other)

    def _ring(self, d, k, s):
        return _copy(self.got[d, k].at[s], self.came[d, k].at[s], self.ring_send.at[d, k, s], self.ring_recv.at[d, k, s],
                     (self.right, self.left)[d])

    def step(self, s, which=(0, 1, 2)):
        for d, k in self.pieces:
            if k not in which:
                continue
            own, got = self.own[d, k], self.got[d, k]
            self._pair(d, k, s).wait_recv()

            @pl.when(s == 0)
            def _():
                got[0] = (own[self._toward(d, 0, self.core)].astype(F32) + got[0].astype(F32)).astype(BF)
                self._ring(d, k, 0).start()

            @pl.when(s > 0)
            def _():
                self._ring(d, k, s - 1).wait_recv()
                total = own[self._toward(d, s, self.core)].astype(F32) + got[s].astype(F32) + self.came[d, k][s - 1].astype(F32)

                @pl.when(s < CHIPS - 1)
                def _():
                    got[s] = total.astype(BF)
                    self._ring(d, k, s).start()

                @pl.when(s == CHIPS - 1)
                def _():
                    self.out[d, k][...] = total.astype(BF)

    def end(self):
        for d, k in self.pieces:
            for s in range(CHIPS):
                self._pair(d, k, s).wait_send()
                if s < CHIPS - 1:
                    self._ring(d, k, s).wait_send()


def _scatter(plan, *refs):
    n, m = len(plan.ins), len(plan.pieces)
    plan.bind(refs[:n], refs[n : n + m], refs[n + m :])
    plan.begin()
    plan.share()
    lax.fori_loop(0, CHIPS, lambda s, _: plan.step(s), None)
    plan.end()


def scatter(layers, collective_id):
    plan = Scatter(layers)
    res = pl.pallas_call(
        functools.partial(_scatter, plan),
        in_specs=plan.in_specs,
        out_specs=plan.out_specs,
        out_shape=plan.out_shape,
        scratch_shapes=plan.scratch,
        compiler_params=pltpu.CompilerParams(collective_id=collective_id, has_side_effects=True, vmem_limit_bytes=VMEM),
        name="scatter",
    )(*plan.ins)
    return plan.results(res)


HOPS = 4
LATE = ((0, 4, 6), (1, 2, 3, 5))
RATE, DELAY = 46e3, 4.5


def _plan(sizes, groups, pieces):
    order = [i for items, _ in groups for i in items]
    due = {i: at for items, at in groups for i in items}
    busy, flying, unsent, now = [0.0, 0.0], [], list(order), 0.0
    slots = [[] for _ in range(len(pieces) + 1)]

    def put(hop, i, d):
        busy[d] = max(busy[d], now) + sizes[i] / RATE
        flying.append((busy[d] + DELAY, hop, i, d))

    def handle(slot, ready):
        for event in ready:
            flying.remove(event)
            _, hop, i, d = event
            slots[slot].append(("pass", hop, i, d))
            if hop + 1 < HOPS or (hop + 1 == HOPS and i % len(NAMES) in LATE[d]):
                put(hop + 1, i, d)

    def feed_links(slot, until):
        while unsent and min(busy) < until:
            i = unsent.pop(0)
            slots[slot].append(("send", i))
            put(1, i, 0)
            put(1, i, 1)

    rank = {i: n for n, i in enumerate(order)}
    for at in range(len(pieces) + 1):
        until = now + (pieces[at] if at < len(pieces) else 0.0)
        while True:
            handle(at, sorted((e for e in flying if e[0] <= now), key=lambda e: (due[e[2]], e[1], rank[e[2]], e[3])))
            feed_links(at, now + DELAY if any(due[i] <= at for i in order if i in unsent or any(e[2] == i for e in flying)) else until + 1)
            needed = [e for e in flying if due[e[2]] <= at or at == len(pieces)]
            if not needed and not (unsent and (due[unsent[0]] <= at or at == len(pieces))):
                break
            if needed:
                now = max(now, min(e[0] for e in (flying if at == len(pieces) else needed)))
            else:
                now += 0.5
        now += pieces[at] if at < len(pieces) else 0.0
    return slots, now


class Gather:
    def __init__(self, own, out, scratch, slots):
        self.own, self.out, self.slots = own, out, slots
        self.ring_send, self.ring_recv, self.pair_send, self.pair_recv, self.local, self.load = scratch
        self.place, self.core = _place()
        self.right, self.left = _member(self.place + 1, self.core), _member(self.place - 1, self.core)
        self.other = _member(self.place, 1 - self.core)
        self.at = 0

    def _block(self, i, member):
        layer, n = divmod(i, len(NAMES))
        rows = self.own[n].shape[1]
        return self.out[n].at[layer, pl.ds(pl.multiple_of(member * rows, rows), rows), :]

    def _away(self, d, hop, core):
        return _member(self.place - hop if d == 0 else self.place + hop, core)

    def _mine(self, i):
        layer, n = divmod(i, len(NAMES))
        return self.own[n].at[layer]

    def _ring(self, d, hop, i):
        dst = self._block(i, self._away(d, hop - 1, self.core))
        return _copy(self._mine(i) if hop == 1 else dst, dst, self.ring_send.at[d, hop - 1, i], self.ring_recv.at[d, hop - 1, i],
                     (self.right, self.left)[d])

    def _came(self, d, hop, i):
        here = self._block(i, self._away(d, hop, self.core))
        return _copy(here, here, self.ring_send.at[d, hop - 1, i], self.ring_recv.at[d, hop - 1, i], (self.right, self.left)[d])

    def _pair(self, slot, i, d, hop, core):
        here = self._block(i, self._away(d, hop, core))
        return _copy(self._mine(i) if slot == 0 else here, here, self.pair_send.at[slot, i], self.pair_recv.at[slot, i], self.other)

    def _keep(self, i):
        return pltpu.make_async_copy(self._mine(i), self._block(i, self._away(0, 0, self.core)), self.local.at[i])

    def begin(self):
        _meet((self.right, self.left, self.other))

    def tick(self):
        for what, *args in self.slots[self.at]:
            if what == "send":
                i = args[0]
                for d in range(2):
                    self._ring(d, 1, i).start()
                self._pair(0, i, 0, 0, self.core).start()
                self._keep(i).start()
            else:
                hop, i, d = args
                self._came(d, hop, i).wait_recv()
                if hop + 1 < HOPS or (hop + 1 == HOPS and i % len(NAMES) in LATE[d]):
                    self._ring(d, hop + 1, i).start()
                self._pair(hop if d == 0 or hop == HOPS else HOPS + hop, i, d, hop, self.core).start()
        self.at += 1

    def _far(self, i):
        for slot in range(CHIPS):
            hop = slot if slot <= HOPS else slot - HOPS
            yield slot, int(slot > HOPS or (slot == HOPS and i % len(NAMES) in LATE[1])), hop

    def fetch(self, i, ref):
        self._whole(i)
        self._fetched(i, ref).start()

    def _whole(self, i):
        self._keep(i).wait()
        for slot, d, hop in self._far(i):
            self._pair(slot, i, d, hop, 1 - self.core).wait_recv()

    def _fetched(self, i, ref):
        layer, n = divmod(i, len(NAMES))
        return pltpu.make_async_copy(self.out[n].at[layer], ref, self.load.at[i])

    def here(self, i, ref):
        self._fetched(i, ref).wait()

    def end(self, rest):
        for i in rest:
            self._whole(i)
        for i in range(self.local.shape[0]):
            for slot, d, hop in self._far(i):
                self._pair(slot, i, d, hop, self.core).wait_send()
                if slot:
                    self._ring(d, hop, i).wait_send()


def _forward(slots, layers, heads, x_ref, cos_ref, sin_ref, *refs):
    n = len(NAMES)
    own, refs = refs[:n], refs[n:]
    whole, h_ref, refs = refs[:n], refs[n], refs[n + 1 :]
    kept, refs = [refs[5 * l : 5 * l + 5] for l in range(layers)], refs[5 * layers :]
    w, comm = refs[:n], Gather(own, whole, refs[n:], slots)
    t = x_ref.shape[0]
    rows = _strip(t)
    comm.begin()
    comm.tick()
    for l in range(layers):
        q_ref, k_ref, v_ref, o_ref, lse_ref = kept[l]
        src = x_ref if l == 0 else h_ref
        for i in range(3):
            comm.fetch(n * l + i, w[i])
        for i in range(3):
            comm.here(n * l + i, w[i])
        for at in range(0, t, rows):
            block = slice(at, at + rows)
            a = _normed(src[block, :])[0].astype(BF)
            cos, sin = cos_ref[block, :], sin_ref[block, :]
            for w_ref, out_ref in zip(w, (q_ref, k_ref, v_ref)):
                r = _nn(a, w_ref[...]).astype(BF)
                for m in range(heads):
                    part = r[:, m * HEAD : (m + 1) * HEAD]
                    out_ref[m, block, :] = part if out_ref is v_ref else _turn(part.astype(F32), cos, sin).astype(BF)
            comm.tick()
        _attend(q_ref, k_ref, v_ref, o_ref, lse_ref, comm.tick)
        if l == layers - 1:
            break
        for i in range(3, n):
            comm.fetch(n * l + i, w[i])
        for i in range(3, n):
            comm.here(n * l + i, w[i])
        for at in range(0, t, rows):
            block = slice(at, at + rows)
            o = jnp.concatenate([o_ref[m, block, :] for m in range(heads)], -1)
            h = (src[block, :].astype(F32) + _nn(o, w[3][...]).astype(BF).astype(F32)).astype(BF)
            b = _normed(h)[0].astype(BF)
            total, step = None, _fit(w[4].shape[1], 512)
            for f in range(0, w[4].shape[1], step):
                gate, up = _nn(b, w[4][:, f : f + step]), _nn(b, w[5][:, f : f + step])
                term = _nn((gate * jax.nn.sigmoid(gate) * up).astype(BF), w[6][f : f + step, :])
                total = term if total is None else total + term
            h_ref[block, :] = (h.astype(F32) + total.astype(BF).astype(F32)).astype(BF)
            comm.tick()
    comm.end([n * (layers - 1) + i for i in range(3, n)])


def forward(x, weights, cos, sin, collective_id):
    n, layers = len(NAMES), weights[0].shape[0]
    t, d = x.shape
    heads = weights[0].shape[2] // HEAD
    whole = [jax.ShapeDtypeStruct((w.shape[0], 2 * CHIPS * w.shape[1], w.shape[2]), BF) for w in weights]
    sizes = {l * n + i: weights[i][0].size * 2 for l in range(layers) for i in range(n)}
    blocks = t // _strip(t)
    project_us, attend_us, feed_us = [1.7] * blocks, [0.45 * (b + 1) for b in range(blocks) for _ in range(heads)], [4.6] * blocks
    pieces, groups = [], []
    for l in range(layers):
        groups.append((range(n * l, n * l + 3), len(pieces)))
        pieces += project_us + attend_us
        groups.append((range(n * l + 3, n * l + n), len(pieces)))
        pieces += feed_us if l < layers - 1 else []
    slots, _ = _plan(sizes, groups, pieces)
    vmem, anywhere, sems = pl.BlockSpec(memory_space=pltpu.VMEM), pl.BlockSpec(memory_space=pl.ANY), pltpu.SemaphoreType.DMA
    head = jax.ShapeDtypeStruct((heads, t, HEAD), BF)
    kept = [head, head, head, head, jax.ShapeDtypeStruct((heads, t), F32)]
    res = pl.pallas_call(
        functools.partial(_forward, slots, layers, heads),
        in_specs=[vmem] * (3 + n),
        out_specs=[anywhere] * n + [vmem] * (1 + 5 * layers),
        out_shape=[*whole, jax.ShapeDtypeStruct((t, d), BF), *kept * layers],
        scratch_shapes=[*[pltpu.VMEM(w.shape[1:], BF) for w in whole], *[sems((2, HOPS, n * layers))] * 2, *[sems((CHIPS, n * layers))] * 2,
                        *[sems((n * layers,))] * 2],
        compiler_params=pltpu.CompilerParams(collective_id=collective_id, has_side_effects=True, vmem_limit_bytes=VMEM),
        name="forward",
    )(x, cos, sin, *weights)
    return res[:n], [x, res[n]], [res[n + 1 + 5 * l : n + 6 + 5 * l] for l in range(layers)]


def solution(mesh):
    def step(x, dy, *arrays):
        weights, m, v = (arrays[i : i + 7] for i in (0, 7, 14))
        layers = weights[0].shape[0]
        cos, sin = tables(x.shape[1])
        whole, states, kept = forward(x[0], weights, cos, sin, 0)
        by_h, terms, mine = dy[0], [None] * layers, [None] * layers
        for number in reversed(range(layers)):
            wq, wk, wv, wo, wg, wu, wd = ((w, number) for w in whole)
            h, (q, k, v_, o, lse) = states[number], kept[number]
            plan = Scatter([terms[number + 1]]) if number + 1 < layers else None
            by_h, do, delta, dwo, dwg, dwu, dwd, *got = feed_back(h, o, by_h, wo, wg, wu, wd, plan, 2 + number)
            if got:
                mine[number + 1] = plan.results(got)[0]
            rest = (by_h, *(w[number] for w in whole[:3])) if number else None
            dwq, dwk, dwv, *by_h = attend_back(q, k, v_, do, lse, delta, h, cos, sin, rest)
            by_h = by_h[0] if by_h else None
            terms[number] = (dwq, dwk, dwv, dwo, dwg, dwu, dwd)
        mine[0] = scatter(terms[:1], 1)[0]
        gradients = [jnp.stack([mine[number][i] for number in range(layers)]).astype(F32) for i in range(7)]
        new = [adamw(w.astype(F32), a, b, g) for w, a, b, g in zip(weights, m, v, gradients, strict=True)]
        return tuple(one[which] for which in range(3) for one in new)

    rows, cut = P(("rep", "dp"), None, None), P(None, "dp", None)
    return jax.shard_map(
        step,
        mesh=mesh,
        in_specs=(rows, rows) + (cut,) * 21,
        out_specs=(P("rep", "dp", None),) * 21,
        check_vma=False,
    )
```
